32 devices in a mesh: aa: 8 (over y, x, core), ba: 4 (over z).
Axes of the slice: x: 2, y: 2, z: 4, core: 2. Of those that a mesh axis runs over, the one named last changes fastest.
Arguments:
- cotangent: bfloat16 [1, 20, 64, 64, 2048], P(None, None, 'aa', 'ba'), may hold values from -6 to 6
- pre_activations: bfloat16 [2, 1, 20, 64, 64, 2048], P(None, None, None, 'aa', 'ba'), may hold values from -6 to 6
- spectral_weights: bfloat16 [2, 2, 20, 20, 24, 6912], P(None, None, None, None, 'ba', 'aa'), may hold values from -6 to 6
- skip_weights: bfloat16 [2, 20, 20], replicated, may hold values from -1.25 to 1.25
- lift_weights: float32 [20], replicated, may hold values from -1.25 to 1.25
Outputs:
- perm_grad: float32 [1, 64, 64, 2048], P(None, 'aa', 'ba')
The draws below stay inside these ranges and needn't reach their ends.
All inputs are finite; a program needn't handle non-finite values.
Results may differ from the reference program's by a relative error of at most 0.023.
Values may be sent and summed in bfloat16 or wider, within the bound.
No kernel may reach another device: no remote copies, remote signals or barrier semaphores. Data moves between devices by JAX's collectives and lax.ppermute only.
A program may use at most 256 MiB of HBM per device.

```python
import math
import jax
import jax.numpy as jnp
from jax import lax

C = 20
NX = 64
NY = 64
NZ = 64
NT = 32
KX = 24
KY = 24
KZ = 24
KT = 12
LAYERS = 2
B = 1


def level_of(key, extent, cuts, smallest, top_value):
    factor_of = 1.0
    for dim, blocks in cuts:
        steps = jax.random.uniform(jax.random.fold_in(jax.random.fold_in(key, 6), dim), (blocks,), jnp.float32, smallest / len(cuts), top_value / len(cuts))
        factor_of = factor_of * jnp.repeat(jnp.exp(steps), extent[dim] // blocks).reshape((-1,) + (1,) * (len(extent) - 1 - dim))
    return factor_of


def normal_values(key, dims, deviation, reach, pieces=(), kind=jnp.bfloat16):
    entries = deviation * jax.random.normal(key, dims, jnp.float32)
    if pieces:
        entries = entries * level_of(key, dims, pieces, -0.22, 0.18)
    return jnp.clip(entries, -reach, reach).astype(kind)


def setup_inputs(seed: int = 0) -> dict:
    key_of = jax.random.split(jax.random.key(seed), 6)
    return {
        "cotangent": normal_values(key_of[0], (B, C, NX, NY, NZ * NT), 1.0, 6.0, ((2, 8), (3, 4))),
        "pre_activations": normal_values(key_of[1], (LAYERS, B, C, NX, NY, NZ * NT), 1.0, 6.0, ((3, 8), (4, 4))),
        "spectral_weights": normal_values(key_of[2], (LAYERS, 2, C, C, KX, KZ * KT * KY), ((NX * NY * NZ * NT) ** 0.5 * (KX * KY * KZ * KT * C) ** -0.5), 6.0, ((4, 4), (5, 8))),
        "skip_weights": normal_values(key_of[3], (LAYERS, C, C), C ** -0.5, 1.25),
        "lift_weights": normal_values(key_of[4], (C,), C ** -0.5, 1.25, (), jnp.float32),
    }


def gelu_slope(values):
    normal_cdf = 0.5 * (1.0 + lax.erf(values / math.sqrt(2.0)))
    density = jnp.exp(-0.5 * values * values) / math.sqrt(2.0 * math.pi)
    return normal_cdf + values * density

def round_complex(values):
    real_part = lax.optimization_barrier(values.real.astype(jnp.bfloat16)).astype(jnp.float32)
    imag_part = lax.optimization_barrier(values.imag.astype(jnp.bfloat16)).astype(jnp.float32)
    return lax.complex(real_part, imag_part)

def kept_index(total_count, length):
    return jnp.concatenate([jnp.arange(total_count // 2, dtype=jnp.int32), jnp.arange(length - total_count // 2, length, dtype=jnp.int32)])

def forward_field(field):
    values = field.astype(jnp.float32).reshape(NX, NY, NZ, NT)
    spectrum = jnp.fft.fft2(values, axes=(2, 3))
    spectrum = jnp.take(spectrum, kept_index(KZ, NZ), axis=2)
    spectrum = round_complex(spectrum[:, :, :, :KT])
    spectrum = round_complex(jnp.take(jnp.fft.fft(spectrum, axis=0), kept_index(KX, NX), axis=0))
    spectrum = round_complex(jnp.take(jnp.fft.fft(spectrum, axis=1), kept_index(KY, NY), axis=1))
    return spectrum

def inverse_field(mode_values, rounded):
    gridded = jnp.zeros((KX, NY, KZ, KT), mode_values.dtype).at[:, kept_index(KY, NY)].set(mode_values)
    gridded = jnp.fft.ifft(gridded, axis=1)
    if rounded:
        gridded = round_complex(gridded)
    spread = jnp.zeros((NX, NY, KZ, KT), mode_values.dtype).at[kept_index(KX, NX)].set(gridded)
    spread = jnp.fft.ifft(spread, axis=0)
    if rounded:
        spread = round_complex(spread)
    plane = jnp.zeros((NX, NY, NZ, NT), mode_values.dtype).at[:, :, kept_index(KZ, NZ), :KT].set(spread)
    return jnp.fft.ifft2(plane, axes=(2, 3)).real.reshape(NX, NY, NZ * NT)

def mix_modes(spectrum, weights):
    shaped = weights.astype(jnp.float32).reshape(2, C, C, KX, KZ, KT, KY)
    conj_weights = lax.complex(shaped[0], -shaped[1])
    return jnp.einsum('oxyzt,oixzty->ixyzt', spectrum, conj_weights)

def sample_grad(cot_sample, pre_sample, spectral_weights, skip_weights, lift_weights):
    incoming = cot_sample.astype(jnp.float32)
    for level_index in range(LAYERS - 1, -1, -1):
        grad_pre = (incoming * gelu_slope(pre_sample[level_index].astype(jnp.float32))).astype(jnp.bfloat16)
        spectrum = lax.map(forward_field, grad_pre)
        mode_values = mix_modes(spectrum, spectral_weights[level_index])
        if level_index > 0:
            mode_values = round_complex(mode_values)
            spectral = lax.map(lambda entry: inverse_field(entry, True), mode_values)
        else:
            spectral = lax.map(lambda entry: inverse_field(entry, False), mode_values)
        skip_term = jnp.einsum('oxyz,oi->ixyz', grad_pre.astype(jnp.float32), skip_weights[level_index].astype(jnp.float32), precision=lax.Precision.HIGHEST)
        incoming = skip_term + spectral
    return jnp.einsum('cxyz,c->xyz', incoming, lift_weights, precision=lax.Precision.HIGHEST)

def reference(cotangent, pre_activations, spectral_weights, skip_weights, lift_weights):

    def one_sample(sample_index):
        cot_sample = lax.dynamic_index_in_dim(cotangent, sample_index, 0, keepdims=False)
        pre_sample = lax.dynamic_index_in_dim(pre_activations, sample_index, 1, keepdims=False)
        return sample_grad(cot_sample, pre_sample, spectral_weights, skip_weights, lift_weights)
    return lax.map(one_sample, jnp.arange(B, dtype=jnp.int32))
```

```python
import functools
import math

import jax
import jax.numpy as jnp
import numpy as np
from jax import lax
from jax.experimental import pallas as pl
from jax.experimental.pallas import tpu as pltpu
from jax.sharding import PartitionSpec as P

NX = 64
NY = 64
NZ = 64
NT = 32
KX = 24
KY = 24
KZ = 24
KT = 12


BF = jnp.bfloat16
F32 = jnp.float32


def signed(count):
    j = np.arange(count)
    return np.where(j < count // 2, j, j - count)


def plane_table():
    kz = np.repeat(signed(KZ), KT)
    kt = np.tile(np.arange(KT), KZ)
    z = np.repeat(np.arange(NZ), NT)
    t = np.tile(np.arange(NT), NZ)
    turns = (np.outer(kz, z) * NT + np.outer(kt, t) * NZ) % (NZ * NT)
    angle = 2.0 * np.pi / (NZ * NT) * turns
    return np.stack([np.cos(angle), -np.sin(angle)], 0)


def line_table(count, length):
    turns = np.outer(np.arange(length), signed(count)) % length
    angle = 2.0 * np.pi / length * turns
    c, s = np.cos(angle), np.sin(angle)
    return np.stack([np.stack([c, -s], 1), np.stack([s, c], 1)], 0)


def slope_of(v):
    cdf = 0.5 * (1.0 + lax.erf(v * (1.0 / math.sqrt(2.0))))
    density = jnp.exp(-0.5 * v * v) * (1.0 / math.sqrt(2.0 * math.pi))
    return cdf + v * density


def nt_dot(a, b):
    return lax.dot_general(a, b, (((1,), (1,)), ((), ())), preferred_element_type=F32)


def nn_dot(a, b):
    return lax.dot_general(a, b, (((1,), (0,)), ((), ())), preferred_element_type=F32)


def full(shape):
    n = len(shape)
    return pl.BlockSpec(shape, lambda *_: (0,) * n)


def params(mib=56, dims=None):
    return pltpu.CompilerParams(vmem_limit_bytes=mib << 20, dimension_semantics=dims)


def cost(flops, nbytes):
    return pl.CostEstimate(flops=int(flops), bytes_accessed=int(nbytes), transcendentals=0)


class Sizes:
    def __init__(self, channels, na, nb):
        self.c = channels
        self.na, self.nb = na, nb
        self.xl, self.yl = NX // na, NY // nb
        self.rows = self.xl * self.yl
        self.m = KZ * KT // na
        self.kx = KX // nb
        self.cells = NZ * NT
        self.g = 4
        units = channels // self.g
        first = (units + 1) // 2
        self.chunks = [(0, first * self.g)]
        if units > first:
            self.chunks.append((first * self.g, (units - first) * self.g))


SLAB = 16


def emit_spectrum(sz, g_rows, table_ref, outs):
    spec = nt_dot(table_ref[...], g_rows)
    per = 2 * sz.m
    for d in range(sz.na):
        for p in range(2):
            lo = d * per + p * sz.m
            part = spec[lo : lo + sz.m]
            pieces = [part[:, k * sz.rows : (k + 1) * sz.rows] for k in range(sz.g)]
            outs[d][p] = jnp.concatenate(pieces, 0).astype(BF)


def first_kernel(sz, cot_ref, pre_ref, table_ref, g_ref, *outs):
    for k in range(sz.g):

        def slab(j, _, k=k):
            s = pl.ds(pl.multiple_of(j * SLAB, SLAB), SLAB)
            v = pre_ref[0, k, s, :].astype(F32)
            g_ref[k, s, :] = (cot_ref[k, s, :].astype(F32) * slope_of(v)).astype(BF)
            return 0

        lax.fori_loop(0, sz.rows // SLAB, slab, 0)
    emit_spectrum(sz, g_ref[...].reshape(sz.g * sz.rows, sz.cells), table_ref, outs)


def first_stage(sz, chunk, cot, pre, layer, table):
    off, cc = chunk
    o = off // sz.g
    blk = (sz.g, sz.rows, sz.cells)
    piece = jax.ShapeDtypeStruct((2, cc * sz.m, sz.rows), BF)
    res = pl.pallas_call(
        functools.partial(first_kernel, sz),
        grid=(cc // sz.g,),
        in_specs=[
            pl.BlockSpec(blk, lambda i: (i + o, 0, 0)),
            pl.BlockSpec((1,) + blk, lambda i: (layer, i + o, 0, 0)),
            full(table.shape),
        ],
        out_specs=[pl.BlockSpec(blk, lambda i: (i, 0, 0))]
        + [pl.BlockSpec((2, sz.g * sz.m, sz.rows), lambda i: (0, i, 0))] * sz.na,
        out_shape=[jax.ShapeDtypeStruct((cc, sz.rows, sz.cells), BF)] + [piece] * sz.na,
        compiler_params=params(),
        cost_estimate=cost(2 * cc * sz.rows * sz.cells * 600, 6 * cc * sz.rows * sz.cells),
        name="first_zt",
    )(cot, pre, table)
    return res[0], list(res[1:])


def skip_kernel(sz, n, *refs):
    g_refs, mat_ref, out_ref = refs[:n], refs[n], refs[n + 1]
    x = jnp.concatenate([r[...] for r in g_refs], 0)
    res = nn_dot(mat_ref[...], x.reshape(sz.c * SLAB, sz.cells))
    out_ref[...] = res.reshape(sz.c, SLAB, sz.cells).astype(BF)


def skip_stage(sz, gs, weight):
    eye = jnp.eye(SLAB, dtype=BF)
    n = sz.c * SLAB
    row = lax.broadcasted_iota(jnp.int32, (n, n), 0)
    col = lax.broadcasted_iota(jnp.int32, (n, n), 1)
    spread = jnp.repeat(jnp.repeat(weight.T, SLAB, 0), SLAB, 1)
    mat = jnp.where(row % SLAB == col % SLAB, spread, jnp.zeros((), BF))
    return pl.pallas_call(
        functools.partial(skip_kernel, sz, len(gs)),
        grid=(sz.rows // SLAB,),
        in_specs=[
            pl.BlockSpec((g.shape[0], SLAB, sz.cells), lambda i: (0, i, 0)) for g in gs
        ]
        + [full((n, n))],
        out_specs=pl.BlockSpec((sz.c, SLAB, sz.cells), lambda i: (0, i, 0)),
        out_shape=jax.ShapeDtypeStruct((sz.c, sz.rows, sz.cells), BF),
        compiler_params=params(),
        cost_estimate=cost(2 * n * n * sz.cells * sz.rows // SLAB, 4 * sz.c * sz.rows * sz.cells),
        name="skip_map",
    )(*gs, mat)


def x_kernel(sz, cc, *refs):
    ins, table_ref, outs = refs[: sz.na], refs[sz.na], refs[sz.na + 1 :]
    x = jnp.concatenate([r[p] for r in ins for p in range(2)], 1)
    res = nn_dot(x, table_ref[...])
    half = cc * sz.m // 2
    w = 2 * sz.kx * sz.yl
    for b in range(sz.nb):
        both = [res[:half, b * w : (b + 1) * w], res[half:, b * w : (b + 1) * w]]
        outs[b][...] = jnp.concatenate(both, 1).astype(BF)


def x_stage(sz, cc, pieces, table):
    w = 2 * sz.kx * sz.yl
    out = jax.ShapeDtypeStruct((cc * sz.m // 2, 2 * w), BF)
    return list(
        pl.pallas_call(
            functools.partial(x_kernel, sz, cc),
            out_shape=[out] * sz.nb,
            compiler_params=params(),
            cost_estimate=cost(2 * cc * sz.m * table.shape[0] * table.shape[1], 8 << 20),
            name="x_forward",
        )(*pieces, table)
    )


def x_back_kernel(sz, cc, *refs):
    ins, table_ref, outs = refs[: sz.nb], refs[sz.nb], refs[sz.nb + 1 :]
    w = 2 * sz.kx * sz.yl
    half = cc * sz.m // 2
    table = table_ref[...]
    for h in range(2):
        x = jnp.concatenate([r[:, h * w : (h + 1) * w] for r in ins], 1)
        res = nt_dot(x, table) * (1.0 / NX)
        for d in range(sz.na):
            for p in range(2):
                k = (d * 2 + p) * sz.rows
                outs[d][p, h * half : (h + 1) * half, :] = res[:, k : k + sz.rows].astype(BF)


def x_back_stage(sz, cc, pieces, table):
    out = jax.ShapeDtypeStruct((2, cc * sz.m, sz.rows), BF)
    return list(
        pl.pallas_call(
            functools.partial(x_back_kernel, sz, cc),
            out_shape=[out] * sz.na,
            compiler_params=params(),
            cost_estimate=cost(2 * cc * sz.m * table.shape[0] * table.shape[1], 8 << 20),
            name="x_backward",
        )(*pieces, table)
    )


ROWS = 16
LANES = 128


def tiles(width):
    return -(-width // LANES)


def put_rows(ref, start, value):
    width = value.shape[1]
    pad = tiles(width) * LANES - width
    if pad:
        value = jnp.concatenate([value, jnp.zeros((value.shape[0], pad), value.dtype)], 1)
    for t in range(tiles(width)):
        ref[(t,) + start] = value[:, t * LANES : (t + 1) * LANES]


def get_rows(ref, start):
    return jnp.concatenate([ref[(t,) + start] for t in range(ref.shape[0])], 1)


def spans(lo, width):
    out = []
    while width:
        t, at = lo // LANES, lo % LANES
        n = min(width, LANES - at)
        out.append((t, at, n))
        lo, width = lo + n, width - n
    return out


def to_lanes(sz, s_ref, z_ref, count):
    groups = 4 * sz.kx
    for m in range(sz.m):
        x = get_rows(s_ref, (pl.ds(m, count, sz.m), slice(None)))
        for k in range(groups):
            at = k * KY
            for t, lo, n in spans(m * KY, KY):
                z_ref[t, k * ROWS : k * ROWS + count, lo : lo + n] = x[:, at : at + n]
                at += n


def from_lanes(sz, z_ref, s_ref, count):
    groups = 4 * sz.kx
    for m in range(sz.m):
        parts = [
            z_ref[t, k * ROWS : k * ROWS + count, lo : lo + n]
            for k in range(groups)
            for t, lo, n in spans(m * KY, KY)
        ]
        put_rows(s_ref, (pl.ds(m, count, sz.m), slice(None)), jnp.concatenate(parts, 1))


def mixed(sz, z_ref, weight_of, t, width):
    where = places(sz)
    acc_re = acc_im = None
    for o in range(sz.c):
        h, r = where[o]
        sr = z_ref[t, pl.ds((2 * h * sz.kx) * ROWS + r, sz.kx, ROWS), :][:, :width]
        si = z_ref[t, pl.ds(((2 * h + 1) * sz.kx) * ROWS + r, sz.kx, ROWS), :][:, :width]
        wr, wi = weight_of(0, o, t * LANES, width), weight_of(1, o, t * LANES, width)
        re = sr * wr + si * wi
        im = si * wr - sr * wi
        acc_re = re if acc_re is None else acc_re + re
        acc_im = im if acc_im is None else acc_im + im
    pad = LANES - width
    if pad:
        zero = jnp.zeros((sz.kx, pad), F32)
        acc_re = jnp.concatenate([acc_re, zero], 1)
        acc_im = jnp.concatenate([acc_im, zero], 1)
    return acc_re, acc_im


def places(sz):
    where, base = {}, 0
    for off, cc in sz.chunks:
        for j in range(cc):
            where[off + j] = (j // (cc // 2), base + j % (cc // 2))
        base += cc // 2
    return where


def load_spectrum(sz, ins, table_ref, s_ref):
    base = 0
    for k, (_, cc) in enumerate(sz.chunks):
        rows = cc * sz.m // 2
        x = jnp.concatenate([ins[k * sz.nb + r][...] for r in range(sz.nb)], 1)
        put_rows(s_ref, (slice(base, base + rows), slice(None)), nn_dot(x, table_ref[...]))
        base += rows


def mix_kernel(sz, *refs):
    n_in = len(sz.chunks) * sz.nb
    ins = refs[:n_in]
    table_ref, w_ref = refs[n_in : n_in + 2]
    outs = refs[n_in + 2 : n_in + 2 + n_in]
    s_ref, z_ref, z2_ref = refs[n_in + 2 + n_in :]
    i = pl.program_id(0)
    where = places(sz)
    count = sz.c // 2

    @pl.when(i == 0)
    def _():
        load_spectrum(sz, ins, table_ref, s_ref)
        to_lanes(sz, s_ref, z_ref, count)

    def weight_of(p, o, lo, width):
        return w_ref[0, p, o, 0, :, lo : lo + width].astype(F32)

    modes = sz.m * KY
    h, r = jnp.int32(0), jnp.int32(0)
    for c in range(sz.c):
        h = jnp.where(i == c, where[c][0], h)
        r = jnp.where(i == c, where[c][1], r)
    for t in range(tiles(modes)):
        re, im = mixed(sz, z_ref, weight_of, t, min(LANES, modes - t * LANES))
        z2_ref[t, pl.ds(2 * h * sz.kx * ROWS + r, sz.kx, ROWS), :] = re
        z2_ref[t, pl.ds((2 * h + 1) * sz.kx * ROWS + r, sz.kx, ROWS), :] = im

    @pl.when(i == sz.c - 1)
    def _():
        from_lanes(sz, z2_ref, s_ref, count)
        w = outs[0].shape[1]
        base = 0
        for k, (_, cc) in enumerate(sz.chunks):
            rows = cc * sz.m // 2
            x = get_rows(s_ref, (slice(base, base + rows), slice(None)))
            x = x[:, : table_ref.shape[1]].astype(BF)
            res = nt_dot(x, table_ref[...]) * (1.0 / NY)
            for r in range(sz.nb):
                outs[k * sz.nb + r][...] = res[:, r * w : (r + 1) * w].astype(BF)
            base += rows


def y_scratch(sz):
    lanes = 4 * sz.kx * KY
    z = pltpu.VMEM((tiles(sz.m * KY), 4 * sz.kx * ROWS, LANES), F32)
    return [pltpu.VMEM((tiles(lanes), sz.c // 2 * sz.m, LANES), F32), z, z]


def mix_stage(sz, pieces, table, weights, layer):
    modes = weights.shape[-1]
    outs = [
        jax.ShapeDtypeStruct((cc * sz.m // 2, 4 * sz.kx * sz.yl), BF)
        for _, cc in sz.chunks
        for _ in range(sz.nb)
    ]
    res = pl.pallas_call(
        functools.partial(mix_kernel, sz),
        grid=(sz.c,),
        in_specs=[full(p.shape) for p in pieces]
        + [
            full(table.shape),
            pl.BlockSpec((1, 2, sz.c, 1, sz.kx, modes), lambda i: (layer, 0, 0, i, 0, 0)),
        ],
        out_specs=[full(s.shape) for s in outs],
        out_shape=outs,
        scratch_shapes=y_scratch(sz),
        compiler_params=params(),
        cost_estimate=cost(20e9, 12 << 20),
        name="y_mix",
    )(*pieces, table, weights)
    n = sz.nb
    return [list(res[k * n : (k + 1) * n]) for k in range(len(sz.chunks))]


def fold_kernel(sz, lift_ref, w_ref, out_ref):
    for p in range(2):
        acc = None
        for i in range(sz.c):
            term = w_ref[0, p, 0, i].astype(F32) * lift_ref[i]
            acc = term if acc is None else acc + term
        out_ref[p, 0] = acc


def fold_stage(sz, weights, lift):
    modes = weights.shape[-1]
    return pl.pallas_call(
        functools.partial(fold_kernel, sz),
        grid=(sz.c,),
        in_specs=[
            pl.BlockSpec(memory_space=pltpu.SMEM),
            pl.BlockSpec((1, 2, 1, sz.c, sz.kx, modes), lambda o: (0, 0, o, 0, 0, 0)),
        ],
        out_specs=pl.BlockSpec((2, 1, sz.kx, modes), lambda o: (0, o, 0, 0)),
        out_shape=jax.ShapeDtypeStruct((2, sz.c, sz.kx, modes), F32),
        compiler_params=params(),
        cost_estimate=cost(6e9, 12 << 20),
        name="fold_lift",
    )(lift, weights)


def mix_last_kernel(sz, *refs):
    n_in = len(sz.chunks) * sz.nb
    ins = refs[:n_in]
    table_ref, w_ref = refs[n_in : n_in + 2]
    outs = refs[n_in + 2 : n_in + 2 + sz.nb]
    s_ref, z_ref, z2_ref = refs[n_in + 2 + sz.nb :]
    load_spectrum(sz, ins, table_ref, s_ref)
    to_lanes(sz, s_ref, z_ref, sz.c // 2)

    def weight_of(p, o, lo, width):
        return w_ref[p, o, :, lo : lo + width]

    modes = sz.m * KY
    z2_ref[...] = jnp.zeros(z2_ref.shape, F32)
    for t in range(tiles(modes)):
        re, im = mixed(sz, z_ref, weight_of, t, min(LANES, modes - t * LANES))
        z2_ref[t, pl.ds(0, sz.kx, ROWS), :] = re
        z2_ref[t, pl.ds(sz.kx * ROWS, sz.kx, ROWS), :] = im
    from_lanes(sz, z2_ref, s_ref, 1)
    w = outs[0].shape[1]
    x = get_rows(s_ref, (slice(0, sz.m), slice(None)))[:, : table_ref.shape[1]]
    res = nt_dot(x.astype(BF), table_ref[...]) * (1.0 / NY)
    for r in range(sz.nb):
        outs[r][...] = res[:, r * w : (r + 1) * w].astype(BF)


def mix_last_stage(sz, pieces, table, folded):
    out = jax.ShapeDtypeStruct((sz.m, 4 * sz.kx * sz.yl), BF)
    return list(
        pl.pallas_call(
            functools.partial(mix_last_kernel, sz),
            out_shape=[out] * sz.nb,
            scratch_shapes=y_scratch(sz),
            compiler_params=params(),
            cost_estimate=cost(4e9, 4 << 20),
            name="y_mix_last",
        )(*pieces, table, folded)
    )


def gather_modes(sz, ins, k):
    parts = [
        r[p].astype(F32)[k * sz.m : (k + 1) * sz.m] for r in ins for p in range(2)
    ]
    return jnp.concatenate(parts, 0)


def next_kernel(sz, v_ref, *refs):
    ins = refs[: sz.na]
    skip_ref, pre_ref, table_ref, part_ref = refs[sz.na : sz.na + 4]
    proj_ref = refs[sz.na + 4]
    outs = refs[sz.na + 5 : sz.na + 5 + sz.na]
    f_ref, g_ref = refs[sz.na + 5 + sz.na :]
    step = pl.program_id(0)
    modes = jnp.concatenate([gather_modes(sz, ins, k) for k in range(sz.g)], 1)
    f_ref[...] = nn_dot(modes.T.astype(BF), table_ref[...]) * (1.0 / sz.cells)

    @pl.when(step == 0)
    def _():
        proj_ref[...] = part_ref[...]

    for k in range(sz.g):
        scale = v_ref[step * sz.g + k]

        def slab(j, _, k=k, scale=scale):
            s = pl.ds(pl.multiple_of(j * SLAB, SLAB), SLAB)
            fs = pl.ds(pl.multiple_of(k * sz.rows + j * SLAB, SLAB), SLAB)
            inc = f_ref[fs, :] + skip_ref[k, s, :].astype(F32)
            g = (inc * slope_of(pre_ref[0, k, s, :].astype(F32))).astype(BF)
            g_ref[fs, :] = g
            proj_ref[s, :] += scale * g.astype(F32)
            return 0

        lax.fori_loop(0, sz.rows // SLAB, slab, 0)
    emit_spectrum(sz, g_ref[...], table_ref, outs)


def next_stage(sz, chunk, pieces, skip, pre, layer, table, lift_skip, partial_proj):
    off, cc = chunk
    o = off // sz.g
    blk = (sz.g, sz.rows, sz.cells)
    piece = jax.ShapeDtypeStruct((2, cc * sz.m, sz.rows), BF)
    pspec = pl.BlockSpec((2, sz.g * sz.m, sz.rows), lambda i: (0, i, 0))
    plane = (sz.rows, sz.cells)
    res = pl.pallas_call(
        functools.partial(next_kernel, sz),
        grid=(cc // sz.g,),
        in_specs=[pl.BlockSpec(memory_space=pltpu.SMEM)]
        + [pspec] * sz.na
        + [
            pl.BlockSpec(blk, lambda i: (i + o, 0, 0)),
            pl.BlockSpec((1,) + blk, lambda i: (layer, i + o, 0, 0)),
            full(table.shape),
            full(plane),
        ],
        out_specs=[full(plane)] + [pspec] * sz.na,
        out_shape=[jax.ShapeDtypeStruct(plane, F32)] + [piece] * sz.na,
        scratch_shapes=[
            pltpu.VMEM((sz.g * sz.rows, sz.cells), F32),
            pltpu.VMEM((sz.g * sz.rows, sz.cells), BF),
        ],
        compiler_params=params(),
        cost_estimate=cost(2 * cc * sz.rows * sz.cells * 1300, 6 * cc * sz.rows * sz.cells),
        name="next_zt",
    )(lift_skip[off : off + cc], *pieces, skip, pre, table, partial_proj)
    return res[0], list(res[1:])


def final_kernel(sz, *refs):
    ins = refs[: sz.na]
    table_ref, proj_ref, out_ref = refs[sz.na :]
    modes = gather_modes(sz, ins, 0)
    spectral = nn_dot(modes.T.astype(BF), table_ref[...]) * (1.0 / sz.cells)
    out_ref[...] = spectral + proj_ref[...]


def final_stage(sz, pieces, table, proj):
    return pl.pallas_call(
        functools.partial(final_kernel, sz),
        out_shape=jax.ShapeDtypeStruct((sz.rows, sz.cells), F32),
        compiler_params=params(),
        cost_estimate=cost(1e9, 6 << 20),
        name="final_zt",
    )(*pieces, table, proj)


def exchange(pieces, axis):
    n = len(pieces)
    return [pieces[0]] + [
        lax.ppermute(pieces[d], axis, [(k, k ^ d) for k in range(n)]) for d in range(1, n)
    ]


def partner(index, d):
    return jnp.bitwise_xor(index, d)


def plane_blocks(sz):
    base = plane_table().reshape(2, sz.na, sz.m, sz.cells).transpose(1, 0, 2, 3)
    const = jnp.asarray(base.reshape(sz.na, 2 * sz.m, sz.cells), BF)
    order = partner(lax.axis_index("aa"), jnp.arange(sz.na, dtype=jnp.int32))
    return jnp.take(const, order, axis=0).reshape(sz.na * 2 * sz.m, sz.cells)


def spread_dot(left, small, right, keep):
    wide = nn_dot(nn_dot(left, small).astype(BF), right)
    return jnp.where(keep, wide, 0.0).astype(BF)


def x_table(sz):
    small = jnp.asarray(line_table(KX, NX).reshape(2 * NX, 2 * KX), BF)
    n, w = sz.na * 2 * sz.rows, sz.nb * 2 * sz.kx * sz.yl
    row = np.arange(n)
    d, p, x = row // (2 * sz.rows), row // sz.rows % 2, row // sz.yl % sz.xl
    place = p * NX + partner(lax.axis_index("aa"), jnp.asarray(d, jnp.int32)) * sz.xl + x
    left = (place[:, None] == jnp.arange(2 * NX)[None, :]).astype(BF)
    col = np.arange(w)
    b, q = col // (2 * sz.kx * sz.yl), col // (sz.kx * sz.yl) % 2
    k = col // sz.yl % sz.kx
    freq = q * KX + partner(lax.axis_index("ba"), jnp.asarray(b, jnp.int32)) * sz.kx + k
    right = (jnp.arange(2 * KX)[:, None] == freq[None, :]).astype(BF)
    keep = (jnp.arange(n) % sz.yl)[:, None] == (jnp.arange(w) % sz.yl)[None, :]
    return spread_dot(left, small, right, keep)


def y_table(sz):
    small = jnp.asarray(line_table(KY, NY).reshape(2 * NY, 2 * KY), BF)
    part = sz.kx * sz.yl
    n, w = sz.nb * 4 * part, 4 * sz.kx * KY
    row = np.arange(n)
    r, h, q = row // (4 * part), row // (2 * part) % 2, row // part % 2
    kx, y = row // sz.yl % sz.kx, row % sz.yl
    place = q * NY + partner(lax.axis_index("ba"), jnp.asarray(r, jnp.int32)) * sz.yl + y
    left = (place[:, None] == jnp.arange(2 * NY)[None, :]).astype(BF)
    col = np.arange(w)
    h2, q2 = col // (2 * sz.kx * KY), col // (sz.kx * KY) % 2
    kx2, ky = col // KY % sz.kx, col % KY
    freq = jnp.asarray(q2 * KY + ky, jnp.int32)
    right = (jnp.arange(2 * KY)[:, None] == freq[None, :]).astype(BF)
    group = jnp.asarray(h * sz.kx + kx, jnp.int32)
    group2 = jnp.asarray(h2 * sz.kx + kx2, jnp.int32)
    return spread_dot(left, small, right, group[:, None] == group2[None, :])


def per_device(cotangent, pre_activations, spectral_weights, skip_weights, lift_weights):
    layers, _, channels, xl, yl, cells = pre_activations.shape
    sz = Sizes(channels, lax.axis_size("aa"), lax.axis_size("ba"))
    plane = plane_blocks(sz)
    tx = x_table(sz)
    ty = y_table(sz)
    pre = pre_activations.reshape(layers, channels, xl * yl, cells)
    cot = cotangent.reshape(channels, xl * yl, cells)
    folded = fold_stage(sz, spectral_weights, lift_weights)
    lift_skip = jnp.sum(skip_weights[0].astype(F32) * lift_weights[None, :], axis=1)

    gs, spectra = [], []
    for chunk in sz.chunks:
        g, pieces = first_stage(sz, chunk, cot, pre, 1, plane)
        gs.append(g)
        spectra.append(exchange(pieces, "aa"))
    skip = skip_stage(sz, gs, skip_weights[1])

    moved = []
    for (_, cc), pieces in zip(sz.chunks, spectra):
        moved += exchange(x_stage(sz, cc, pieces, tx), "ba")
    modes = mix_stage(sz, moved, ty, spectral_weights, 1)

    back = []
    for (_, cc), pieces in zip(sz.chunks, modes):
        back.append(exchange(x_back_stage(sz, cc, exchange(pieces, "ba"), tx), "aa"))

    proj = jnp.zeros((sz.rows, cells), F32)
    spectra = []
    for chunk, pieces in zip(sz.chunks, back):
        proj, out = next_stage(sz, chunk, pieces, skip, pre, 0, plane, lift_skip, proj)
        spectra.append(exchange(out, "aa"))

    moved = []
    for (_, cc), pieces in zip(sz.chunks, spectra):
        moved += exchange(x_stage(sz, cc, pieces, tx), "ba")
    last = exchange(mix_last_stage(sz, moved, ty, folded), "ba")
    last = exchange(x_back_stage(sz, 2, last, tx), "aa")
    out = final_stage(sz, last, plane, proj)
    return out.reshape(1, xl, yl, cells)


def solution(mesh):
    return jax.shard_map(
        per_device,
        mesh=mesh,
        in_specs=(
            P(None, None, "aa", "ba", None),
            P(None, None, None, "aa", "ba", None),
            P(None, None, None, None, "ba", "aa"),
            P(),
            P(),
        ),
        out_specs=P(None, "aa", "ba", None),
        check_vma=False,
    )
```

```python
import functools
import math

import jax
import jax.numpy as jnp
import numpy as np
from jax import lax
from jax.experimental import pallas as pl
from jax.experimental.pallas import tpu as pltpu
from jax.sharding import PartitionSpec as P

NX = 64
NY = 64
NZ = 64
NT = 32
KX = 24
KY = 24
KZ = 24
KT = 12


STACKED = {"aa": False, "ba": False}

BF = jnp.bfloat16
F32 = jnp.float32


def signed(count):
    j = np.arange(count)
    return np.where(j < count // 2, j, j - count)


def plane_table():
    kz = np.repeat(signed(KZ), KT)
    kt = np.tile(np.arange(KT), KZ)
    z = np.repeat(np.arange(NZ), NT)
    t = np.tile(np.arange(NT), NZ)
    turns = (np.outer(kz, z) * NT + np.outer(kt, t) * NZ) % (NZ * NT)
    angle = 2.0 * np.pi / (NZ * NT) * turns
    return np.stack([np.cos(angle), -np.sin(angle)], 0)


def line_table(count, length):
    turns = np.outer(np.arange(length), signed(count)) % length
    angle = 2.0 * np.pi / length * turns
    c, s = np.cos(angle), np.sin(angle)
    return np.stack([np.stack([c, -s], 1), np.stack([s, c], 1)], 0)


def slope_of(v):
    cdf = 0.5 * (1.0 + lax.erf(v * (1.0 / math.sqrt(2.0))))
    density = jnp.exp(-0.5 * v * v) * (1.0 / math.sqrt(2.0 * math.pi))
    return cdf + v * density


def nt_dot(a, b):
    return lax.dot_general(a, b, (((1,), (1,)), ((), ())), preferred_element_type=F32)


def nn_dot(a, b):
    return lax.dot_general(a, b, (((1,), (0,)), ((), ())), preferred_element_type=F32)


def full(shape):
    n = len(shape)
    return pl.BlockSpec(shape, lambda *_: (0,) * n)


def params(mib=40, dims=None):
    return pltpu.CompilerParams(vmem_limit_bytes=mib << 20, dimension_semantics=dims)


def cost(flops, nbytes):
    return pl.CostEstimate(flops=int(flops), bytes_accessed=int(nbytes), transcendentals=0)


def count_of(axis, n):
    return 1 if STACKED[axis] else n


def parts_of(refs, axis, n):
    return [refs[0].at[d] for d in range(n)] if STACKED[axis] else list(refs)


def shapes_of(axis, n, shape):
    if STACKED[axis]:
        return [jax.ShapeDtypeStruct((n,) + shape, BF)]
    return [jax.ShapeDtypeStruct(shape, BF)] * n


def specs_of(axis, n, block):
    if STACKED[axis]:
        return [pl.BlockSpec((n,) + block, lambda i: (0, 0, i, 0))]
    return [pl.BlockSpec(block, lambda i: (0, i, 0))] * n


VM = pl.BlockSpec(memory_space=pltpu.VMEM)


class Sizes:
    def __init__(self, channels, na, nb):
        self.c = channels
        self.na, self.nb = na, nb
        self.xl, self.yl = NX // na, NY // nb
        self.rows = self.xl * self.yl
        self.m = KZ * KT // na
        self.kx = KX // nb
        self.cells = NZ * NT
        self.g = 4
        units = channels // self.g
        first = (units + 1) // 2
        self.ca, self.cb = count_of("aa", na), count_of("ba", nb)
        self.chunks = [(0, first * self.g)]
        if units > first:
            self.chunks.append((first * self.g, (units - first) * self.g))


SLAB = 16


def emit_spectrum(sz, g_rows, table_ref, outs):
    spec = nt_dot(table_ref[...], g_rows)
    per = 2 * sz.m
    for d in range(sz.na):
        for p in range(2):
            lo = d * per + p * sz.m
            part = spec[lo : lo + sz.m]
            pieces = [part[:, k * sz.rows : (k + 1) * sz.rows] for k in range(sz.g)]
            outs[d][p] = jnp.concatenate(pieces, 0).astype(BF)


def first_kernel(sz, cot_ref, pre_ref, table_ref, g_ref, *outs):
    for k in range(sz.g):

        def slab(j, _, k=k):
            s = pl.ds(pl.multiple_of(j * SLAB, SLAB), SLAB)
            v = pre_ref[0, k, s, :].astype(F32)
            g_ref[k, s, :] = (cot_ref[k, s, :].astype(F32) * slope_of(v)).astype(BF)
            return 0

        lax.fori_loop(0, sz.rows // SLAB, slab, 0)
    outs = parts_of(outs, "aa", sz.na)
    emit_spectrum(sz, g_ref[...].reshape(sz.g * sz.rows, sz.cells), table_ref, outs)


def first_stage(sz, chunk, cot, pre, layer, table):
    off, cc = chunk
    o = off // sz.g
    blk = (sz.g, sz.rows, sz.cells)
    res = pl.pallas_call(
        functools.partial(first_kernel, sz),
        grid=(cc // sz.g,),
        in_specs=[
            pl.BlockSpec(blk, lambda i: (i + o, 0, 0)),
            pl.BlockSpec((1,) + blk, lambda i: (layer, i + o, 0, 0)),
            full(table.shape),
        ],
        out_specs=[pl.BlockSpec(blk, lambda i: (i, 0, 0))]
        + specs_of("aa", sz.na, (2, sz.g * sz.m, sz.rows)),
        out_shape=[jax.ShapeDtypeStruct((cc, sz.rows, sz.cells), BF)]
        + shapes_of("aa", sz.na, (2, cc * sz.m, sz.rows)),
        compiler_params=params(),
        cost_estimate=cost(2 * cc * sz.rows * sz.cells * 600, 6 * cc * sz.rows * sz.cells),
        name="first_zt",
    )(cot, pre, table)
    return res[0], list(res[1:])


def skip_kernel(sz, n, *refs):
    g_refs, mat_ref, out_ref = refs[:n], refs[n], refs[n + 1]
    x = jnp.concatenate([r[...] for r in g_refs], 0)
    res = nn_dot(mat_ref[...], x.reshape(sz.c * SLAB, sz.cells))
    out_ref[...] = res.reshape(sz.c, SLAB, sz.cells).astype(BF)


def skip_stage(sz, gs, weight):
    eye = jnp.eye(SLAB, dtype=BF)
    n = sz.c * SLAB
    row = lax.broadcasted_iota(jnp.int32, (n, n), 0)
    col = lax.broadcasted_iota(jnp.int32, (n, n), 1)
    spread = jnp.repeat(jnp.repeat(weight.T, SLAB, 0), SLAB, 1)
    mat = jnp.where(row % SLAB == col % SLAB, spread, jnp.zeros((), BF))
    return pl.pallas_call(
        functools.partial(skip_kernel, sz, len(gs)),
        grid=(sz.rows // SLAB,),
        in_specs=[
            pl.BlockSpec((g.shape[0], SLAB, sz.cells), lambda i: (0, i, 0)) for g in gs
        ]
        + [full((n, n))],
        out_specs=pl.BlockSpec((sz.c, SLAB, sz.cells), lambda i: (0, i, 0)),
        out_shape=jax.ShapeDtypeStruct((sz.c, sz.rows, sz.cells), BF),
        compiler_params=params(),
        cost_estimate=cost(2 * n * n * sz.cells * sz.rows // SLAB, 4 * sz.c * sz.rows * sz.cells),
        name="skip_map",
    )(*gs, mat)


def x_kernel(sz, cc, *refs):
    ins, table_ref = parts_of(refs, "aa", sz.na)[: sz.na], refs[sz.ca]
    outs = parts_of(refs[sz.ca + 1 :], "ba", sz.nb)
    x = jnp.concatenate([r[p] for r in ins for p in range(2)], 1)
    res = nn_dot(x, table_ref[...])
    half = cc * sz.m // 2
    w = 2 * sz.kx * sz.yl
    for b in range(sz.nb):
        both = [res[:half, b * w : (b + 1) * w], res[half:, b * w : (b + 1) * w]]
        outs[b][...] = jnp.concatenate(both, 1).astype(BF)


def x_stage(sz, cc, pieces, table):
    w = 2 * sz.kx * sz.yl
    return list(
        pl.pallas_call(
            functools.partial(x_kernel, sz, cc),
            in_specs=[VM] * (sz.ca + 1),
            out_specs=[VM] * sz.cb,
            out_shape=shapes_of("ba", sz.nb, (cc * sz.m // 2, 2 * w)),
            compiler_params=params(16),
            cost_estimate=cost(2 * cc * sz.m * table.shape[0] * table.shape[1], 8 << 20),
            name="x_forward",
        )(*pieces, table)
    )


def x_back_kernel(sz, cc, *refs):
    ins, table_ref = parts_of(refs, "ba", sz.nb)[: sz.nb], refs[sz.cb]
    outs = parts_of(refs[sz.cb + 1 :], "aa", sz.na)
    w = 2 * sz.kx * sz.yl
    half = cc * sz.m // 2
    table = table_ref[...]
    for h in range(2):
        x = jnp.concatenate([r[:, h * w : (h + 1) * w] for r in ins], 1)
        res = nt_dot(x, table) * (1.0 / NX)
        for d in range(sz.na):
            for p in range(2):
                k = (d * 2 + p) * sz.rows
                outs[d][p, h * half : (h + 1) * half, :] = res[:, k : k + sz.rows].astype(BF)


def x_back_stage(sz, cc, pieces, table):
    return list(
        pl.pallas_call(
            functools.partial(x_back_kernel, sz, cc),
            in_specs=[VM] * (sz.cb + 1),
            out_specs=[VM] * sz.ca,
            out_shape=shapes_of("aa", sz.na, (2, cc * sz.m, sz.rows)),
            compiler_params=params(16),
            cost_estimate=cost(2 * cc * sz.m * table.shape[0] * table.shape[1], 8 << 20),
            name="x_backward",
        )(*pieces, table)
    )


ROWS = 16
LANES = 128


def tiles(width):
    return -(-width // LANES)


def put_rows(ref, start, value):
    width = value.shape[1]
    pad = tiles(width) * LANES - width
    if pad:
        value = jnp.concatenate([value, jnp.zeros((value.shape[0], pad), value.dtype)], 1)
    for t in range(tiles(width)):
        ref[(t,) + start] = value[:, t * LANES : (t + 1) * LANES]


def get_rows(ref, start):
    return jnp.concatenate([ref[(t,) + start] for t in range(ref.shape[0])], 1)


def spans(lo, width):
    out = []
    while width:
        t, at = lo // LANES, lo % LANES
        n = min(width, LANES - at)
        out.append((t, at, n))
        lo, width = lo + n, width - n
    return out


def to_lanes(sz, s_ref, z_ref, count):
    groups = 4 * sz.kx
    for m in range(sz.m):
        x = get_rows(s_ref, (pl.ds(m, count, sz.m), slice(None)))
        for k in range(groups):
            at = k * KY
            for t, lo, n in spans(m * KY, KY):
                z_ref[t, k * ROWS : k * ROWS + count, lo : lo + n] = x[:, at : at + n]
                at += n


def from_lanes(sz, z_ref, s_ref, count):
    groups = 4 * sz.kx
    for m in range(sz.m):
        parts = [
            z_ref[t, k * ROWS : k * ROWS + count, lo : lo + n]
            for k in range(groups)
            for t, lo, n in spans(m * KY, KY)
        ]
        put_rows(s_ref, (pl.ds(m, count, sz.m), slice(None)), jnp.concatenate(parts, 1))


def places(sz):
    where, base = {}, 0
    for off, cc in sz.chunks:
        for j in range(cc):
            where[off + j] = (j // (cc // 2), base + j % (cc // 2))
        base += cc // 2
    return where


def load_spectrum(sz, ins, table_ref, s_ref, z_ref, d_ref):
    base = 0
    for k, (_, cc) in enumerate(sz.chunks):
        rows = cc * sz.m // 2
        pieces = parts_of(ins[k * sz.cb : (k + 1) * sz.cb], "ba", sz.nb)
        x = jnp.concatenate([r[...] for r in pieces], 1)
        put_rows(s_ref, (slice(base, base + rows), slice(None)), nn_dot(x, table_ref[...]))
        base += rows
    z_ref[...] = jnp.zeros(z_ref.shape, F32)
    to_lanes(sz, s_ref, z_ref, sz.c // 2)
    for o, (h, r) in places(sz).items():
        for q in range(2):
            for t in range(tiles(sz.m * KY)):
                rows = pl.ds(((2 * h + q) * sz.kx) * ROWS + r, SUB, ROWS)
                d_ref[q, t, o] = z_ref[t, rows, :]


def mixed(sz, d_ref, weight_of, t, fields):
    acc = [None] * fields
    for o in range(sz.c):
        sr, si = d_ref[0, t, o], d_ref[1, t, o]
        for f in range(fields):
            wr, wi = weight_of(0, o, f, t), weight_of(1, o, f, t)
            re = sr * wr + si * wi
            im = si * wr - sr * wi
            acc[f] = (re, im) if acc[f] is None else (acc[f][0] + re, acc[f][1] + im)
    return acc


FIELDS = 4


def mix_kernel(sz, *refs):
    n_in = len(sz.chunks) * sz.cb
    ins = refs[:n_in]
    table_ref, w_ref = refs[n_in : n_in + 2]
    outs = refs[n_in + 2 : n_in + 2 + n_in]
    s_ref, z_ref, d_ref, z2_ref = refs[n_in + 2 + n_in :]
    i = pl.program_id(0)
    where = places(sz)

    @pl.when(i == 0)
    def _():
        load_spectrum(sz, ins, table_ref, s_ref, z_ref, d_ref)

    def weight_of(p, o, f, t):
        return w_ref[p, o, f, :, t * LANES : (t + 1) * LANES].astype(F32)

    starts = []
    for f in range(FIELDS):
        at = jnp.int32(0)
        for step in range(sz.c // FIELDS):
            h, r = where[step * FIELDS + f]
            at = jnp.where(i == step, 2 * h * sz.kx * ROWS + r, at)
        starts.append(at)
    for t in range(tiles(sz.m * KY)):
        for f, (re, im) in enumerate(mixed(sz, d_ref, weight_of, t, FIELDS)):
            z2_ref[t, pl.ds(starts[f], sz.kx, ROWS), :] = re[: sz.kx]
            z2_ref[t, pl.ds(starts[f] + sz.kx * ROWS, sz.kx, ROWS), :] = im[: sz.kx]

    @pl.when(i == sz.c // FIELDS - 1)
    def _():
        from_lanes(sz, z2_ref, s_ref, sz.c // 2)
        w = 4 * sz.kx * sz.yl
        base = 0
        for k, (_, cc) in enumerate(sz.chunks):
            rows = cc * sz.m // 2
            x = get_rows(s_ref, (slice(base, base + rows), slice(None)))
            x = x[:, : table_ref.shape[1]].astype(BF)
            res = nt_dot(x, table_ref[...]) * (1.0 / NY)
            pieces = parts_of(outs[k * sz.cb : (k + 1) * sz.cb], "ba", sz.nb)
            for r in range(sz.nb):
                pieces[r][...] = res[:, r * w : (r + 1) * w].astype(BF)
            base += rows


SUB = 8


def y_scratch(sz):
    lanes = 4 * sz.kx * KY
    wide = tiles(sz.m * KY)
    z = pltpu.VMEM((wide, (4 * sz.kx + SUB) * ROWS, LANES), F32)
    return [
        pltpu.VMEM((tiles(lanes), sz.c // 2 * sz.m, LANES), F32),
        z,
        pltpu.VMEM((2, wide, sz.c, SUB, LANES), F32),
        z,
    ]


def pad_tiles(sz, weights):
    lead = [(0, 0)] * (weights.ndim - 2)
    over = tiles(sz.m * KY) * LANES - weights.shape[-1]
    return jnp.pad(weights, lead + [(0, SUB - sz.kx), (0, over)])


def mix_stage(sz, pieces, table, weights):
    modes = weights.shape[-1]
    outs = []
    for _, cc in sz.chunks:
        outs += shapes_of("ba", sz.nb, (cc * sz.m // 2, 4 * sz.kx * sz.yl))
    res = pl.pallas_call(
        functools.partial(mix_kernel, sz),
        grid=(sz.c // FIELDS,),
        in_specs=[VM] * (len(pieces) + 1)
        + [pl.BlockSpec((2, sz.c, FIELDS, SUB, modes), lambda i: (0, 0, i, 0, 0))],
        out_specs=[VM] * len(outs),
        out_shape=outs,
        scratch_shapes=y_scratch(sz),
        compiler_params=params(24),
        cost_estimate=cost(20e9, 12 << 20),
        name="y_mix",
    )(*pieces, table, weights)
    n = sz.cb
    return [list(res[k * n : (k + 1) * n]) for k in range(len(sz.chunks))]


def mix_last_kernel(sz, *refs):
    n_in = len(sz.chunks) * sz.cb
    ins = refs[:n_in]
    table_ref, w_ref = refs[n_in : n_in + 2]
    outs = refs[n_in + 2 : n_in + 2 + sz.cb]
    s_ref, z_ref, d_ref, z2_ref = refs[n_in + 2 + sz.cb :]
    load_spectrum(sz, ins, table_ref, s_ref, z_ref, d_ref)

    def weight_of(p, o, f, t):
        return w_ref[p, o, :, t * LANES : (t + 1) * LANES]

    z2_ref[...] = jnp.zeros(z2_ref.shape, F32)
    for t in range(tiles(sz.m * KY)):
        re, im = mixed(sz, d_ref, weight_of, t, 1)[0]
        z2_ref[t, pl.ds(0, sz.kx, ROWS), :] = re[: sz.kx]
        z2_ref[t, pl.ds(sz.kx * ROWS, sz.kx, ROWS), :] = im[: sz.kx]
    from_lanes(sz, z2_ref, s_ref, 1)
    w = 4 * sz.kx * sz.yl
    x = get_rows(s_ref, (slice(0, sz.m), slice(None)))[:, : table_ref.shape[1]]
    res = nt_dot(x.astype(BF), table_ref[...]) * (1.0 / NY)
    pieces = parts_of(outs, "ba", sz.nb)
    for r in range(sz.nb):
        pieces[r][...] = res[:, r * w : (r + 1) * w].astype(BF)


def mix_last_stage(sz, pieces, table, folded):
    return list(
        pl.pallas_call(
            functools.partial(mix_last_kernel, sz),
            in_specs=[VM] * (len(pieces) + 2),
            out_specs=[VM] * sz.cb,
            out_shape=shapes_of("ba", sz.nb, (sz.m, 4 * sz.kx * sz.yl)),
            scratch_shapes=y_scratch(sz),
            compiler_params=params(24),
            cost_estimate=cost(4e9, 4 << 20),
            name="y_mix_last",
        )(*pieces, table, folded)
    )


def gather_modes(sz, ins, k):
    parts = [
        r[p].astype(F32)[k * sz.m : (k + 1) * sz.m] for r in ins for p in range(2)
    ]
    return jnp.concatenate(parts, 0)


def next_kernel(sz, v_ref, *refs):
    n = sz.ca
    ins = parts_of(refs[:n], "aa", sz.na)
    skip_ref, pre_ref, table_ref, part_ref = refs[n : n + 4]
    proj_ref = refs[n + 4]
    outs = parts_of(refs[n + 5 : n + 5 + n], "aa", sz.na)
    f_ref, g_ref = refs[n + 5 + n :]
    step = pl.program_id(0)
    modes = jnp.concatenate([gather_modes(sz, ins, k) for k in range(sz.g)], 1)
    f_ref[...] = nn_dot(modes.T.astype(BF), table_ref[...]) * (1.0 / sz.cells)

    @pl.when(step == 0)
    def _():
        proj_ref[...] = part_ref[...]

    for k in range(sz.g):
        scale = v_ref[step * sz.g + k]

        def slab(j, _, k=k, scale=scale):
            s = pl.ds(pl.multiple_of(j * SLAB, SLAB), SLAB)
            fs = pl.ds(pl.multiple_of(k * sz.rows + j * SLAB, SLAB), SLAB)
            inc = f_ref[fs, :] + skip_ref[k, s, :].astype(F32)
            g = (inc * slope_of(pre_ref[0, k, s, :].astype(F32))).astype(BF)
            g_ref[fs, :] = g
            proj_ref[s, :] += scale * g.astype(F32)
            return 0

        lax.fori_loop(0, sz.rows // SLAB, slab, 0)
    emit_spectrum(sz, g_ref[...], table_ref, outs)


def next_stage(sz, chunk, pieces, skip, pre, layer, table, lift_skip, partial_proj):
    off, cc = chunk
    o = off // sz.g
    blk = (sz.g, sz.rows, sz.cells)
    pspecs = specs_of("aa", sz.na, (2, sz.g * sz.m, sz.rows))
    plane = (sz.rows, sz.cells)
    res = pl.pallas_call(
        functools.partial(next_kernel, sz),
        grid=(cc // sz.g,),
        in_specs=[pl.BlockSpec(memory_space=pltpu.SMEM)]
        + pspecs
        + [
            pl.BlockSpec(blk, lambda i: (i + o, 0, 0)),
            pl.BlockSpec((1,) + blk, lambda i: (layer, i + o, 0, 0)),
            full(table.shape),
            full(plane),
        ],
        out_specs=[full(plane)] + pspecs,
        out_shape=[jax.ShapeDtypeStruct(plane, F32)]
        + shapes_of("aa", sz.na, (2, cc * sz.m, sz.rows)),
        scratch_shapes=[
            pltpu.VMEM((sz.g * sz.rows, sz.cells), F32),
            pltpu.VMEM((sz.g * sz.rows, sz.cells), BF),
        ],
        compiler_params=params(),
        cost_estimate=cost(2 * cc * sz.rows * sz.cells * 1300, 6 * cc * sz.rows * sz.cells),
        name="next_zt",
    )(lift_skip[off : off + cc], *pieces, skip, pre, table, partial_proj)
    return res[0], list(res[1:])


def final_kernel(sz, *refs):
    ins = parts_of(refs[: sz.ca], "aa", sz.na)
    table_ref, proj_ref, out_ref = refs[sz.ca :]
    modes = gather_modes(sz, ins, 0)
    spectral = nn_dot(modes.T.astype(BF), table_ref[...]) * (1.0 / sz.cells)
    out_ref[...] = spectral + proj_ref[...]


def final_stage(sz, pieces, table, proj):
    return pl.pallas_call(
        functools.partial(final_kernel, sz),
        in_specs=[VM] * (sz.ca + 2),
        out_specs=VM,
        out_shape=jax.ShapeDtypeStruct((sz.rows, sz.cells), F32),
        compiler_params=params(),
        cost_estimate=cost(1e9, 6 << 20),
        name="final_zt",
    )(*pieces, table, proj)


def exchange(pieces, axis):
    if STACKED[axis]:
        return [lax.all_to_all(pieces[0], axis, split_axis=0, concat_axis=0, tiled=True)]
    n = len(pieces)
    return [pieces[0]] + [
        lax.ppermute(pieces[d], axis, [(k, k ^ d) for k in range(n)]) for d in range(1, n)
    ]


def partner(axis, d):
    d = jnp.asarray(d, jnp.int32)
    return d if STACKED[axis] else jnp.bitwise_xor(lax.axis_index(axis), d)


def plane_blocks(sz):
    base = plane_table().reshape(2, sz.na, sz.m, sz.cells).transpose(1, 0, 2, 3)
    const = jnp.asarray(base.reshape(sz.na, 2 * sz.m, sz.cells), BF)
    if not STACKED["aa"]:
        const = jnp.take(const, partner("aa", np.arange(sz.na)), axis=0)
    return const.reshape(sz.na * 2 * sz.m, sz.cells)


def spread_dot(left, small, right, keep):
    wide = nn_dot(nn_dot(left, small).astype(BF), right)
    return jnp.where(keep, wide, 0.0).astype(BF)


def x_table(sz):
    small = jnp.asarray(line_table(KX, NX).reshape(2 * NX, 2 * KX), BF)
    n, w = sz.na * 2 * sz.rows, sz.nb * 2 * sz.kx * sz.yl
    row = np.arange(n)
    d, p, x = row // (2 * sz.rows), row // sz.rows % 2, row // sz.yl % sz.xl
    place = p * NX + partner("aa", d) * sz.xl + x
    left = (place[:, None] == jnp.arange(2 * NX)[None, :]).astype(BF)
    col = np.arange(w)
    b, q = col // (2 * sz.kx * sz.yl), col // (sz.kx * sz.yl) % 2
    k = col // sz.yl % sz.kx
    freq = q * KX + partner("ba", b) * sz.kx + k
    right = (jnp.arange(2 * KX)[:, None] == freq[None, :]).astype(BF)
    keep = (jnp.arange(n) % sz.yl)[:, None] == (jnp.arange(w) % sz.yl)[None, :]
    return spread_dot(left, small, right, keep)


def y_table(sz):
    small = jnp.asarray(line_table(KY, NY).reshape(2 * NY, 2 * KY), BF)
    part = sz.kx * sz.yl
    n, w = sz.nb * 4 * part, 4 * sz.kx * KY
    row = np.arange(n)
    r, h, q = row // (4 * part), row // (2 * part) % 2, row // part % 2
    kx, y = row // sz.yl % sz.kx, row % sz.yl
    place = q * NY + partner("ba", r) * sz.yl + y
    left = (place[:, None] == jnp.arange(2 * NY)[None, :]).astype(BF)
    col = np.arange(w)
    h2, q2 = col // (2 * sz.kx * KY), col // (sz.kx * KY) % 2
    kx2, ky = col // KY % sz.kx, col % KY
    freq = jnp.asarray(q2 * KY + ky, jnp.int32)
    right = (jnp.arange(2 * KY)[:, None] == freq[None, :]).astype(BF)
    group = jnp.asarray(h * sz.kx + kx, jnp.int32)
    group2 = jnp.asarray(h2 * sz.kx + kx2, jnp.int32)
    return spread_dot(left, small, right, group[:, None] == group2[None, :])


def per_device(cotangent, pre_activations, spectral_weights, skip_weights, lift_weights):
    layers, _, channels, xl, yl, cells = pre_activations.shape
    sz = Sizes(channels, lax.axis_size("aa"), lax.axis_size("ba"))
    plane = plane_blocks(sz)
    tx = x_table(sz)
    ty = y_table(sz)
    pre = pre_activations.reshape(layers, channels, xl * yl, cells)
    cot = cotangent.reshape(channels, xl * yl, cells)
    lift = lift_weights[None, None, :, None, None]
    folded = pad_tiles(sz, jnp.sum(spectral_weights[0].astype(F32) * lift, axis=2))
    weights = pad_tiles(sz, spectral_weights[1])
    lift_skip = jnp.sum(skip_weights[0].astype(F32) * lift_weights[None, :], axis=1)

    gs, spectra = [], []
    for chunk in sz.chunks:
        g, pieces = first_stage(sz, chunk, cot, pre, 1, plane)
        gs.append(g)
        spectra.append(exchange(pieces, "aa"))
    skip = skip_stage(sz, gs, skip_weights[1])

    moved = []
    for (_, cc), pieces in zip(sz.chunks, spectra):
        moved += exchange(x_stage(sz, cc, pieces, tx), "ba")
    modes = mix_stage(sz, moved, ty, weights)

    back = []
    for (_, cc), pieces in zip(sz.chunks, modes):
        back.append(exchange(x_back_stage(sz, cc, exchange(pieces, "ba"), tx), "aa"))

    proj = jnp.zeros((sz.rows, cells), F32)
    spectra = []
    for chunk, pieces in zip(sz.chunks, back):
        proj, out = next_stage(sz, chunk, pieces, skip, pre, 0, plane, lift_skip, proj)
        spectra.append(exchange(out, "aa"))

    moved = []
    for (_, cc), pieces in zip(sz.chunks, spectra):
        moved += exchange(x_stage(sz, cc, pieces, tx), "ba")
    last = exchange(mix_last_stage(sz, moved, ty, folded), "ba")
    last = exchange(x_back_stage(sz, 2, last, tx), "aa")
    out = final_stage(sz, last, plane, proj)
    return out.reshape(1, xl, yl, cells)


def solution(mesh):
    return jax.shard_map(
        per_device,
        mesh=mesh,
        in_specs=(
            P(None, None, "aa", "ba", None),
            P(None, None, None, "aa", "ba", None),
            P(None, None, None, None, "ba", "aa"),
            P(),
            P(),
        ),
        out_specs=P(None, "aa", "ba", None),
        check_vma=False,
    )
```

```python
import functools
import math

import jax
import jax.numpy as jnp
import numpy as np
from jax import lax
from jax.experimental import pallas as pl
from jax.experimental.pallas import tpu as pltpu
from jax.sharding import PartitionSpec as P


NX = 64
NY = 64
NZ = 64
NT = 32
KX = 24
KY = 24
KZ = 24
KT = 12


BF = jnp.bfloat16
F32 = jnp.float32


def signed(count):
    j = np.arange(count)
    return np.where(j < count // 2, j, j - count)


def plane_table():
    kz = np.repeat(signed(KZ), KT)
    kt = np.tile(np.arange(KT), KZ)
    z = np.repeat(np.arange(NZ), NT)
    t = np.tile(np.arange(NT), NZ)
    turns = (np.outer(kz, z) * NT + np.outer(kt, t) * NZ) % (NZ * NT)
    angle = 2.0 * np.pi / (NZ * NT) * turns
    return np.stack([np.cos(angle), -np.sin(angle)], 0)


def line_table(count, length):
    turns = np.outer(np.arange(length), signed(count)) % length
    angle = 2.0 * np.pi / length * turns
    c, s = np.cos(angle), np.sin(angle)
    return np.stack([np.stack([c, -s], 1), np.stack([s, c], 1)], 0)


def slope_of(v):
    cdf = 0.5 * (1.0 + lax.erf(v * (1.0 / math.sqrt(2.0))))
    density = jnp.exp(-0.5 * v * v) * (1.0 / math.sqrt(2.0 * math.pi))
    return cdf + v * density


def nt_dot(a, b):
    return lax.dot_general(a, b, (((1,), (1,)), ((), ())), preferred_element_type=F32)


def nn_dot(a, b):
    return lax.dot_general(a, b, (((1,), (0,)), ((), ())), preferred_element_type=F32)


def full(shape):
    n = len(shape)
    return pl.BlockSpec(shape, lambda *_: (0,) * n)


def params(mib=40, dims=None):
    return pltpu.CompilerParams(vmem_limit_bytes=mib << 20, dimension_semantics=dims)


def cost(flops, nbytes):
    return pl.CostEstimate(flops=int(flops), bytes_accessed=int(nbytes), transcendentals=0)


def parts_of(refs):
    return list(refs)


def shapes_of(n, shape):
    return [jax.ShapeDtypeStruct(shape, BF)] * n


def specs_of(n, block):
    return [pl.BlockSpec(block, lambda i: (0, i, 0))] * n


VM = pl.BlockSpec(memory_space=pltpu.VMEM)


class Sizes:
    def __init__(self, channels, na, nb):
        self.c = channels
        self.na, self.nb = na, nb
        self.xl, self.yl = NX // na, NY // nb
        self.rows = self.xl * self.yl
        self.m = KZ * KT // na
        self.kx = KX // nb
        self.cells = NZ * NT
        self.g = 4
        units = channels // self.g
        first = (units + 1) // 2
        self.ca, self.cb = na, nb
        self.chunks = [(0, first * self.g)]
        if units > first:
            self.chunks.append((first * self.g, (units - first) * self.g))


SLAB = 16


def emit_spectrum(sz, g_rows, table_ref, outs):
    spec = nt_dot(table_ref[...], g_rows)
    per = 2 * sz.m
    for d in range(sz.na):
        for p in range(2):
            lo = d * per + p * sz.m
            part = spec[lo : lo + sz.m]
            pieces = [part[:, k * sz.rows : (k + 1) * sz.rows] for k in range(sz.g)]
            outs[d][p] = jnp.concatenate(pieces, 0).astype(BF)


def first_kernel(sz, cot_ref, pre_ref, table_ref, after_ref, g_ref, *outs):
    for k in range(sz.g):

        def slab(j, _, k=k):
            s = pl.ds(pl.multiple_of(j * SLAB, SLAB), SLAB)
            v = pre_ref[0, k, s, :].astype(F32)
            g_ref[k, s, :] = (cot_ref[k, s, :].astype(F32) * slope_of(v)).astype(BF)
            return 0

        lax.fori_loop(0, sz.rows // SLAB, slab, 0)
    outs = parts_of(outs)
    emit_spectrum(sz, g_ref[...].reshape(sz.g * sz.rows, sz.cells), table_ref, outs)


def first_stage(sz, chunk, cot, pre, layer, table, after):
    off, cc = chunk
    o = off // sz.g
    blk = (sz.g, sz.rows, sz.cells)
    res = pl.pallas_call(
        functools.partial(first_kernel, sz),
        grid=(cc // sz.g,),
        in_specs=[
            pl.BlockSpec(blk, lambda i: (i + o, 0, 0)),
            pl.BlockSpec((1,) + blk, lambda i: (layer, i + o, 0, 0)),
            full(table.shape),
            pl.BlockSpec(memory_space=pl.ANY),
        ],
        out_specs=[pl.BlockSpec(blk, lambda i: (i, 0, 0))]
        + specs_of(sz.na, (2, sz.g * sz.m, sz.rows)),
        out_shape=[jax.ShapeDtypeStruct((cc, sz.rows, sz.cells), BF)]
        + shapes_of(sz.na, (2, cc * sz.m, sz.rows)),
        compiler_params=params(),
        cost_estimate=cost(2 * cc * sz.rows * sz.cells * 600, 6 * cc * sz.rows * sz.cells),
        name="first_zt",
    )(cot, pre, table, after)
    return res[0], list(res[1:])


def skip_kernel(sz, n, *refs):
    g_refs, mat_ref, out_ref = refs[:n], refs[n], refs[n + 1]
    x = jnp.concatenate([r[...] for r in g_refs], 0)
    res = nn_dot(mat_ref[...], x.reshape(sz.c * SLAB, sz.cells))
    out_ref[...] = res.reshape(sz.c, SLAB, sz.cells).astype(BF)


def skip_stage(sz, gs, weight):
    eye = jnp.eye(SLAB, dtype=BF)
    n = sz.c * SLAB
    row = lax.broadcasted_iota(jnp.int32, (n, n), 0)
    col = lax.broadcasted_iota(jnp.int32, (n, n), 1)
    spread = jnp.repeat(jnp.repeat(weight.T, SLAB, 0), SLAB, 1)
    mat = jnp.where(row % SLAB == col % SLAB, spread, jnp.zeros((), BF))
    return pl.pallas_call(
        functools.partial(skip_kernel, sz, len(gs)),
        grid=(sz.rows // SLAB,),
        in_specs=[
            pl.BlockSpec((g.shape[0], SLAB, sz.cells), lambda i: (0, i, 0)) for g in gs
        ]
        + [full((n, n))],
        out_specs=pl.BlockSpec((sz.c, SLAB, sz.cells), lambda i: (0, i, 0)),
        out_shape=jax.ShapeDtypeStruct((sz.c, sz.rows, sz.cells), BF),
        compiler_params=params(),
        cost_estimate=cost(2 * n * n * sz.cells * sz.rows // SLAB, 4 * sz.c * sz.rows * sz.cells),
        name="skip_map",
    )(*gs, mat)


def x_kernel(sz, cc, *refs):
    ins, table_ref = parts_of(refs)[: sz.na], refs[sz.ca]
    outs = parts_of(refs[sz.ca + 1 :])
    x = jnp.concatenate([r[p] for r in ins for p in range(2)], 1)
    res = nn_dot(x, table_ref[...])
    half = cc * sz.m // 2
    w = 2 * sz.kx * sz.yl
    for b in range(sz.nb):
        both = [res[:half, b * w : (b + 1) * w], res[half:, b * w : (b + 1) * w]]
        outs[b][...] = jnp.concatenate(both, 1).astype(BF)


def x_stage(sz, cc, pieces, table):
    w = 2 * sz.kx * sz.yl
    return list(
        pl.pallas_call(
            functools.partial(x_kernel, sz, cc),
            in_specs=[VM] * (sz.ca + 1),
            out_specs=[VM] * sz.cb,
            out_shape=shapes_of(sz.nb, (cc * sz.m // 2, 2 * w)),
            compiler_params=params(16),
            cost_estimate=cost(2 * cc * sz.m * table.shape[0] * table.shape[1], 8 << 20),
            name="x_forward",
        )(*pieces, table)
    )


def x_back_kernel(sz, cc, *refs):
    ins, table_ref = parts_of(refs)[: sz.nb], refs[sz.cb]
    outs = parts_of(refs[sz.cb + 1 :])
    w = 2 * sz.kx * sz.yl
    half = cc * sz.m // 2
    table = table_ref[...]
    for h in range(2):
        x = jnp.concatenate([r[:, h * w : (h + 1) * w] for r in ins], 1)
        res = nt_dot(x, table) * (1.0 / NX)
        for d in range(sz.na):
            for p in range(2):
                k = (d * 2 + p) * sz.rows
                outs[d][p, h * half : (h + 1) * half, :] = res[:, k : k + sz.rows].astype(BF)


def x_back_stage(sz, cc, pieces, table):
    return list(
        pl.pallas_call(
            functools.partial(x_back_kernel, sz, cc),
            in_specs=[VM] * (sz.cb + 1),
            out_specs=[VM] * sz.ca,
            out_shape=shapes_of(sz.na, (2, cc * sz.m, sz.rows)),
            compiler_params=params(16),
            cost_estimate=cost(2 * cc * sz.m * table.shape[0] * table.shape[1], 8 << 20),
            name="x_backward",
        )(*pieces, table)
    )


ROWS = 16
LANES = 128


def tiles(width):
    return -(-width // LANES)


def put_rows(ref, start, value):
    width = value.shape[1]
    pad = tiles(width) * LANES - width
    if pad:
        value = jnp.concatenate([value, jnp.zeros((value.shape[0], pad), value.dtype)], 1)
    for t in range(tiles(width)):
        ref[(t,) + start] = value[:, t * LANES : (t + 1) * LANES]


def get_rows(ref, start):
    return jnp.concatenate([ref[(t,) + start] for t in range(ref.shape[0])], 1)


def spans(lo, width):
    out = []
    while width:
        t, at = lo // LANES, lo % LANES
        n = min(width, LANES - at)
        out.append((t, at, n))
        lo, width = lo + n, width - n
    return out


def to_lanes(sz, s_ref, z_ref, count):
    groups = 4 * sz.kx
    for m in range(sz.m):
        x = get_rows(s_ref, (pl.ds(m, count, sz.m), slice(None)))
        for k in range(groups):
            at = k * KY
            for t, lo, n in spans(m * KY, KY):
                z_ref[t, k * ROWS : k * ROWS + count, lo : lo + n] = x[:, at : at + n]
                at += n


def from_lanes(sz, z_ref, s_ref, count):
    groups = 4 * sz.kx
    for m in range(sz.m):
        parts = [
            z_ref[t, k * ROWS : k * ROWS + count, lo : lo + n]
            for k in range(groups)
            for t, lo, n in spans(m * KY, KY)
        ]
        put_rows(s_ref, (pl.ds(m, count, sz.m), slice(None)), jnp.concatenate(parts, 1))


def places(sz):
    where, base = {}, 0
    for off, cc in sz.chunks:
        for j in range(cc):
            where[off + j] = (j // (cc // 2), base + j % (cc // 2))
        base += cc // 2
    return where


def load_spectrum(sz, ins, table_ref, s_ref, z_ref, d_ref):
    base = 0
    for k, (_, cc) in enumerate(sz.chunks):
        rows = cc * sz.m // 2
        pieces = parts_of(ins[k * sz.cb : (k + 1) * sz.cb])
        x = jnp.concatenate([r[...] for r in pieces], 1)
        put_rows(s_ref, (slice(base, base + rows), slice(None)), nn_dot(x, table_ref[...]))
        base += rows
    z_ref[...] = jnp.zeros(z_ref.shape, F32)
    to_lanes(sz, s_ref, z_ref, sz.c // 2)
    for o, (h, r) in places(sz).items():
        for q in range(2):
            for t in range(tiles(sz.m * KY)):
                rows = pl.ds(((2 * h + q) * sz.kx) * ROWS + r, SUB, ROWS)
                d_ref[q, t, o] = z_ref[t, rows, :]


def mixed(sz, d_ref, weight_of, t, fields):
    acc = [None] * fields
    for o in range(sz.c):
        sr, si = d_ref[0, t, o], d_ref[1, t, o]
        for f in range(fields):
            wr, wi = weight_of(0, o, f, t), weight_of(1, o, f, t)
            re = sr * wr + si * wi
            im = si * wr - sr * wi
            acc[f] = (re, im) if acc[f] is None else (acc[f][0] + re, acc[f][1] + im)
    return acc


FIELDS = 4


def mix_kernel(sz, *refs):
    n_in = len(sz.chunks) * sz.cb
    ins = refs[:n_in]
    table_ref, w_ref = refs[n_in : n_in + 2]
    outs = refs[n_in + 2 : n_in + 2 + n_in]
    s_ref, z_ref, d_ref, z2_ref = refs[n_in + 2 + n_in :]
    i = pl.program_id(0)
    where = places(sz)

    @pl.when(i == 0)
    def _():
        load_spectrum(sz, ins, table_ref, s_ref, z_ref, d_ref)

    def weight_of(p, o, f, t):
        return w_ref[p, o, f, :, t * LANES : (t + 1) * LANES].astype(F32)

    starts = []
    for f in range(FIELDS):
        at = jnp.int32(0)
        for step in range(sz.c // FIELDS):
            h, r = where[step * FIELDS + f]
            at = jnp.where(i == step, 2 * h * sz.kx * ROWS + r, at)
        starts.append(at)
    for t in range(tiles(sz.m * KY)):
        for f, (re, im) in enumerate(mixed(sz, d_ref, weight_of, t, FIELDS)):
            z2_ref[t, pl.ds(starts[f], sz.kx, ROWS), :] = re[: sz.kx]
            z2_ref[t, pl.ds(starts[f] + sz.kx * ROWS, sz.kx, ROWS), :] = im[: sz.kx]

    @pl.when(i == sz.c // FIELDS - 1)
    def _():
        from_lanes(sz, z2_ref, s_ref, sz.c // 2)
        w = 4 * sz.kx * sz.yl
        base = 0
        for k, (_, cc) in enumerate(sz.chunks):
            rows = cc * sz.m // 2
            x = get_rows(s_ref, (slice(base, base + rows), slice(None)))
            x = x[:, : table_ref.shape[1]].astype(BF)
            res = nt_dot(x, table_ref[...]) * (1.0 / NY)
            pieces = parts_of(outs[k * sz.cb : (k + 1) * sz.cb])
            for r in range(sz.nb):
                pieces[r][...] = res[:, r * w : (r + 1) * w].astype(BF)
            base += rows


SUB = 8


def y_scratch(sz):
    lanes = 4 * sz.kx * KY
    wide = tiles(sz.m * KY)
    z = pltpu.VMEM((wide, (4 * sz.kx + SUB) * ROWS, LANES), F32)
    return [
        pltpu.VMEM((tiles(lanes), sz.c // 2 * sz.m, LANES), F32),
        z,
        pltpu.VMEM((2, wide, sz.c, SUB, LANES), F32),
        z,
    ]


def pad_tiles(sz, weights):
    lead = [(0, 0)] * (weights.ndim - 2)
    over = tiles(sz.m * KY) * LANES - weights.shape[-1]
    return jnp.pad(weights, lead + [(0, SUB - sz.kx), (0, over)])


def mix_stage(sz, pieces, table, weights):
    modes = weights.shape[-1]
    outs = []
    for _, cc in sz.chunks:
        outs += shapes_of(sz.nb, (cc * sz.m // 2, 4 * sz.kx * sz.yl))
    res = pl.pallas_call(
        functools.partial(mix_kernel, sz),
        grid=(sz.c // FIELDS,),
        in_specs=[VM] * (len(pieces) + 1)
        + [pl.BlockSpec((2, sz.c, FIELDS, SUB, modes), lambda i: (0, 0, i, 0, 0))],
        out_specs=[VM] * len(outs),
        out_shape=outs,
        scratch_shapes=y_scratch(sz),
        compiler_params=params(24),
        cost_estimate=cost(20e9, 12 << 20),
        name="y_mix",
    )(*pieces, table, weights)
    n = sz.cb
    return [list(res[k * n : (k + 1) * n]) for k in range(len(sz.chunks))]


def mix_last_kernel(sz, *refs):
    n_in = len(sz.chunks) * sz.cb
    ins = refs[:n_in]
    table_ref, w_ref = refs[n_in : n_in + 2]
    outs = refs[n_in + 2 : n_in + 2 + sz.cb]
    s_ref, z_ref, d_ref, z2_ref = refs[n_in + 2 + sz.cb :]
    load_spectrum(sz, ins, table_ref, s_ref, z_ref, d_ref)

    def weight_of(p, o, f, t):
        return w_ref[p, o, :, t * LANES : (t + 1) * LANES]

    z2_ref[...] = jnp.zeros(z2_ref.shape, F32)
    for t in range(tiles(sz.m * KY)):
        re, im = mixed(sz, d_ref, weight_of, t, 1)[0]
        z2_ref[t, pl.ds(0, sz.kx, ROWS), :] = re[: sz.kx]
        z2_ref[t, pl.ds(sz.kx * ROWS, sz.kx, ROWS), :] = im[: sz.kx]
    from_lanes(sz, z2_ref, s_ref, 1)
    w = 4 * sz.kx * sz.yl
    x = get_rows(s_ref, (slice(0, sz.m), slice(None)))[:, : table_ref.shape[1]]
    res = nt_dot(x.astype(BF), table_ref[...]) * (1.0 / NY)
    pieces = parts_of(outs)
    for r in range(sz.nb):
        pieces[r][...] = res[:, r * w : (r + 1) * w].astype(BF)


def mix_last_stage(sz, pieces, table, folded):
    return list(
        pl.pallas_call(
            functools.partial(mix_last_kernel, sz),
            in_specs=[VM] * (len(pieces) + 2),
            out_specs=[VM] * sz.cb,
            out_shape=shapes_of(sz.nb, (sz.m, 4 * sz.kx * sz.yl)),
            scratch_shapes=y_scratch(sz),
            compiler_params=params(24),
            cost_estimate=cost(4e9, 4 << 20),
            name="y_mix_last",
        )(*pieces, table, folded)
    )


def gather_modes(sz, ins, k):
    parts = [
        r[p].astype(F32)[k * sz.m : (k + 1) * sz.m] for r in ins for p in range(2)
    ]
    return jnp.concatenate(parts, 0)


def next_kernel(sz, v_ref, *refs):
    n = sz.ca
    ins = parts_of(refs[:n])
    skip_ref, pre_ref, table_ref, part_ref = refs[n : n + 4]
    proj_ref = refs[n + 4]
    outs = parts_of(refs[n + 5 : n + 5 + n])
    f_ref, g_ref = refs[n + 5 + n :]
    step = pl.program_id(0)
    modes = jnp.concatenate([gather_modes(sz, ins, k) for k in range(sz.g)], 1)
    f_ref[...] = nn_dot(modes.T.astype(BF), table_ref[...]) * (1.0 / sz.cells)

    @pl.when(step == 0)
    def _():
        proj_ref[...] = part_ref[...]

    for k in range(sz.g):
        scale = v_ref[step * sz.g + k]

        def slab(j, _, k=k, scale=scale):
            s = pl.ds(pl.multiple_of(j * SLAB, SLAB), SLAB)
            fs = pl.ds(pl.multiple_of(k * sz.rows + j * SLAB, SLAB), SLAB)
            inc = f_ref[fs, :] + skip_ref[k, s, :].astype(F32)
            g = (inc * slope_of(pre_ref[0, k, s, :].astype(F32))).astype(BF)
            g_ref[fs, :] = g
            proj_ref[s, :] += scale * g.astype(F32)
            return 0

        lax.fori_loop(0, sz.rows // SLAB, slab, 0)
    emit_spectrum(sz, g_ref[...], table_ref, outs)


def next_stage(sz, chunk, pieces, skip, pre, layer, table, lift_skip, partial_proj):
    off, cc = chunk
    o = off // sz.g
    blk = (sz.g, sz.rows, sz.cells)
    pspecs = specs_of(sz.na, (2, sz.g * sz.m, sz.rows))
    plane = (sz.rows, sz.cells)
    res = pl.pallas_call(
        functools.partial(next_kernel, sz),
        grid=(cc // sz.g,),
        in_specs=[pl.BlockSpec(memory_space=pltpu.SMEM)]
        + pspecs
        + [
            pl.BlockSpec(blk, lambda i: (i + o, 0, 0)),
            pl.BlockSpec((1,) + blk, lambda i: (layer, i + o, 0, 0)),
            full(table.shape),
            full(plane),
        ],
        out_specs=[full(plane)] + pspecs,
        out_shape=[jax.ShapeDtypeStruct(plane, F32)]
        + shapes_of(sz.na, (2, cc * sz.m, sz.rows)),
        scratch_shapes=[
            pltpu.VMEM((sz.g * sz.rows, sz.cells), F32),
            pltpu.VMEM((sz.g * sz.rows, sz.cells), BF),
        ],
        compiler_params=params(),
        cost_estimate=cost(2 * cc * sz.rows * sz.cells * 1300, 6 * cc * sz.rows * sz.cells),
        name="next_zt",
    )(lift_skip[off : off + cc], *pieces, skip, pre, table, partial_proj)
    return res[0], list(res[1:])


def final_kernel(sz, *refs):
    ins = parts_of(refs[: sz.ca])
    table_ref, proj_ref, out_ref = refs[sz.ca :]
    modes = gather_modes(sz, ins, 0)
    spectral = nn_dot(modes.T.astype(BF), table_ref[...]) * (1.0 / sz.cells)
    out_ref[...] = spectral + proj_ref[...]


def final_stage(sz, pieces, table, proj):
    return pl.pallas_call(
        functools.partial(final_kernel, sz),
        in_specs=[VM] * (sz.ca + 2),
        out_specs=VM,
        out_shape=jax.ShapeDtypeStruct((sz.rows, sz.cells), F32),
        compiler_params=params(),
        cost_estimate=cost(1e9, 6 << 20),
        name="final_zt",
    )(*pieces, table, proj)


def exchange(pieces, axis):
    n = len(pieces)
    out = [pieces[0]]
    for d in range(1, n):
        out.append(lax.ppermute(pieces[d], axis, [(k, k ^ d) for k in range(n)]))
    return out


def partner(axis, d):
    return jnp.bitwise_xor(lax.axis_index(axis), jnp.asarray(d, jnp.int32))


def plane_blocks(sz):
    base = plane_table().reshape(2, sz.na, sz.m, sz.cells).transpose(1, 0, 2, 3)
    const = jnp.asarray(base.reshape(sz.na, 2 * sz.m, sz.cells), BF)
    const = jnp.take(const, partner("aa", np.arange(sz.na)), axis=0)
    return const.reshape(sz.na * 2 * sz.m, sz.cells)


def spread_dot(left, small, right, keep):
    wide = nn_dot(nn_dot(left, small).astype(BF), right)
    return jnp.where(keep, wide, 0.0).astype(BF)


def x_table(sz):
    small = jnp.asarray(line_table(KX, NX).reshape(2 * NX, 2 * KX), BF)
    n, w = sz.na * 2 * sz.rows, sz.nb * 2 * sz.kx * sz.yl
    row = np.arange(n)
    d, p, x = row // (2 * sz.rows), row // sz.rows % 2, row // sz.yl % sz.xl
    place = p * NX + partner("aa", d) * sz.xl + x
    left = (place[:, None] == jnp.arange(2 * NX)[None, :]).astype(BF)
    col = np.arange(w)
    b, q = col // (2 * sz.kx * sz.yl), col // (sz.kx * sz.yl) % 2
    k = col // sz.yl % sz.kx
    freq = q * KX + partner("ba", b) * sz.kx + k
    right = (jnp.arange(2 * KX)[:, None] == freq[None, :]).astype(BF)
    keep = (jnp.arange(n) % sz.yl)[:, None] == (jnp.arange(w) % sz.yl)[None, :]
    return spread_dot(left, small, right, keep)


def y_table(sz, zero):
    small = jnp.asarray(line_table(KY, NY).reshape(2 * NY, 2 * KY), BF) + zero
    part = sz.kx * sz.yl
    n, w = sz.nb * 4 * part, 4 * sz.kx * KY
    row = np.arange(n)
    r, h, q = row // (4 * part), row // (2 * part) % 2, row // part % 2
    kx, y = row // sz.yl % sz.kx, row % sz.yl
    place = q * NY + partner("ba", r) * sz.yl + y
    left = (place[:, None] == jnp.arange(2 * NY)[None, :]).astype(BF)
    col = np.arange(w)
    h2, q2 = col // (2 * sz.kx * KY), col // (sz.kx * KY) % 2
    kx2, ky = col // KY % sz.kx, col % KY
    freq = jnp.asarray(q2 * KY + ky, jnp.int32)
    right = (jnp.arange(2 * KY)[:, None] == freq[None, :]).astype(BF)
    group = jnp.asarray(h * sz.kx + kx, jnp.int32)
    group2 = jnp.asarray(h2 * sz.kx + kx2, jnp.int32)
    return spread_dot(left, small, right, group[:, None] == group2[None, :])


def whole(cotangent, pre_activations, spectral_weights, skip_weights, lift_weights):
    layers, _, channels, xl, yl, cells = pre_activations.shape
    sz = Sizes(channels, lax.axis_size("aa"), lax.axis_size("ba"))
    plane = plane_blocks(sz)
    tx = x_table(sz)
    pre = pre_activations.reshape(layers, channels, xl * yl, cells)
    cot = cotangent.reshape(channels, xl * yl, cells)
    lift_skip = jnp.sum(skip_weights[0].astype(F32) * lift_weights[None, :], axis=1)

    gs, spectra = [], []
    after = lift_skip
    for chunk in sz.chunks:
        g, pieces = first_stage(sz, chunk, cot, pre, 1, plane, after)
        after = g
        gs.append(g)
        spectra.append(exchange(pieces, "aa"))
    skip = skip_stage(sz, gs, skip_weights[1])

    moved = []
    for (_, cc), pieces in zip(sz.chunks, spectra):
        out = x_stage(sz, cc, pieces, tx)
        moved.append(exchange(out, "ba"))
        last_out = out[0]
    raw, zero, _ = lax.optimization_barrier(
        (spectral_weights[1], jnp.zeros((), BF), last_out)
    )
    weights = pad_tiles(sz, raw)
    ty = y_table(sz, zero)
    modes = mix_stage(sz, sum(moved, []), ty, weights)

    back = [exchange(pieces, "ba") for pieces in modes]
    for j, ((_, cc), pieces) in enumerate(zip(sz.chunks, back)):
        out = x_back_stage(sz, cc, pieces, tx)
        back[j] = exchange(out, "aa")

    lift = lift_weights[None, None, :, None, None]
    folded = pad_tiles(sz, jnp.sum(spectral_weights[0].astype(F32) * lift, axis=2))
    proj = jnp.zeros((sz.rows, cells), F32)
    spectra = []
    for chunk, pieces in zip(sz.chunks, back):
        proj, out = next_stage(sz, chunk, pieces, skip, pre, 0, plane, lift_skip, proj)
        spectra.append(exchange(out, "aa"))

    moved = []
    for (_, cc), pieces in zip(sz.chunks, spectra):
        out = x_stage(sz, cc, pieces, tx)
        moved += exchange(out, "ba")
    last = exchange(mix_last_stage(sz, moved, ty, folded), "ba")
    last = exchange(x_back_stage(sz, 2, last, tx), "aa")
    out = final_stage(sz, last, plane, proj)
    return out.reshape(1, xl, yl, cells)


def solution(mesh):
    return jax.shard_map(
        whole,
        mesh=mesh,
        in_specs=(
            P(None, None, "aa", "ba", None),
            P(None, None, None, "aa", "ba", None),
            P(None, None, None, None, "ba", "aa"),
            P(),
            P(),
        ),
        out_specs=P(None, "aa", "ba", None),
        check_vma=False,
    )
```

```python
import functools
import math

import jax
import jax.numpy as jnp
import numpy as np
from jax import lax
from jax.experimental import pallas as pl
from jax.experimental.pallas import tpu as pltpu
from jax.sharding import PartitionSpec as P


NX = 64
NY = 64
NZ = 64
NT = 32
KX = 24
KY = 24
KZ = 24
KT = 12


BF = jnp.bfloat16
F32 = jnp.float32


def signed(count):
    j = np.arange(count)
    return np.where(j < count // 2, j, j - count)


def plane_factors():
    kz = np.repeat(signed(KZ), KT)
    kt = np.tile(np.arange(KT), KZ)
    a = 2.0 * np.pi / NZ * (np.outer(kz, np.arange(NZ)) % NZ)
    b = 2.0 * np.pi / NT * (np.outer(kt, np.arange(NT)) % NT)
    b = np.pad(b, ((0, 0), (0, NZ - NT)))
    first = np.stack([np.cos(a), -np.sin(a)], 0), np.stack([np.cos(b)] * 2, 0)
    second = np.stack([np.sin(a), np.cos(a)], 0), np.stack([-np.sin(b)] * 2, 0)
    wide = []
    for f in first + second:
        coarse = f.astype(BF)
        wide += [coarse, (f - coarse.astype(np.float64)).astype(BF)]
    return np.concatenate(wide, 2)


def line_table(count, length):
    turns = np.outer(np.arange(length), signed(count)) % length
    angle = 2.0 * np.pi / length * turns
    c, s = np.cos(angle), np.sin(angle)
    return np.stack([np.stack([c, -s], 1), np.stack([s, c], 1)], 0)


def slope_of(v):
    cdf = 0.5 * (1.0 + lax.erf(v * (1.0 / math.sqrt(2.0))))
    density = jnp.exp(-0.5 * v * v) * (1.0 / math.sqrt(2.0 * math.pi))
    return cdf + v * density


def nt_dot(a, b):
    return lax.dot_general(a, b, (((1,), (1,)), ((), ())), preferred_element_type=F32)


def nn_dot(a, b):
    return lax.dot_general(a, b, (((1,), (0,)), ((), ())), preferred_element_type=F32)


def full(shape):
    n = len(shape)
    return pl.BlockSpec(shape, lambda *_: (0,) * n)


def params(mib=40, dims=None):
    return pltpu.CompilerParams(vmem_limit_bytes=mib << 20, dimension_semantics=dims)


def cost(flops, nbytes):
    return pl.CostEstimate(flops=int(flops), bytes_accessed=int(nbytes), transcendentals=0)


def parts_of(refs):
    return list(refs)


def shapes_of(n, shape):
    return [jax.ShapeDtypeStruct(shape, BF)] * n


def specs_of(n, block):
    return [pl.BlockSpec(block, lambda i: (0, i, 0))] * n


VM = pl.BlockSpec(memory_space=pltpu.VMEM)


class Sizes:
    def __init__(self, channels, na, nb):
        self.c = channels
        self.na, self.nb = na, nb
        self.xl, self.yl = NX // na, NY // nb
        self.rows = self.xl * self.yl
        self.m = KZ * KT // na
        self.kx = KX // nb
        self.cells = NZ * NT
        self.g = 4
        units = channels // self.g
        first = (units + 1) // 2
        self.ca, self.cb = na, nb
        self.chunks = [(0, first * self.g)]
        if units > first:
            self.chunks.append((first * self.g, (units - first) * self.g))


SLAB = 16


def emit_spectrum(sz, g_rows, table_ref, outs):
    spec = nt_dot(table_ref[...], g_rows)
    per = 2 * sz.m
    for d in range(sz.na):
        for p in range(2):
            lo = d * per + p * sz.m
            part = spec[lo : lo + sz.m]
            pieces = [part[:, k * sz.rows : (k + 1) * sz.rows] for k in range(sz.g)]
            outs[d][p] = jnp.concatenate(pieces, 0).astype(BF)


def first_kernel(sz, cot_ref, pre_ref, table_ref, after_ref, g_ref, *outs):
    for k in range(sz.g):

        def slab(j, _, k=k):
            s = pl.ds(pl.multiple_of(j * SLAB, SLAB), SLAB)
            v = pre_ref[0, k, s, :].astype(F32)
            g_ref[k, s, :] = (cot_ref[k, s, :].astype(F32) * slope_of(v)).astype(BF)
            return 0

        lax.fori_loop(0, sz.rows // SLAB, slab, 0)
    outs = parts_of(outs)
    emit_spectrum(sz, g_ref[...].reshape(sz.g * sz.rows, sz.cells), table_ref, outs)


def first_stage(sz, chunk, cot, pre, layer, table, after):
    off, cc = chunk
    o = off // sz.g
    blk = (sz.g, sz.rows, sz.cells)
    res = pl.pallas_call(
        functools.partial(first_kernel, sz),
        grid=(cc // sz.g,),
        in_specs=[
            pl.BlockSpec(blk, lambda i: (i + o, 0, 0)),
            pl.BlockSpec((1,) + blk, lambda i: (layer, i + o, 0, 0)),
            full(table.shape),
            pl.BlockSpec(memory_space=pl.ANY),
        ],
        out_specs=[pl.BlockSpec(blk, lambda i: (i, 0, 0))]
        + specs_of(sz.na, (2, sz.g * sz.m, sz.rows)),
        out_shape=[jax.ShapeDtypeStruct((cc, sz.rows, sz.cells), BF)]
        + shapes_of(sz.na, (2, cc * sz.m, sz.rows)),
        compiler_params=params(),
        cost_estimate=cost(2 * cc * sz.rows * sz.cells * 600, 6 * cc * sz.rows * sz.cells),
        name="first_zt",
    )(cot, pre, table, after)
    return res[0], list(res[1:])


def skip_kernel(sz, n, *refs):
    g_refs, mat_ref, out_ref = refs[:n], refs[n], refs[n + 1]
    x = jnp.concatenate([r[...] for r in g_refs], 0)
    res = nn_dot(mat_ref[...], x.reshape(sz.c * SLAB, sz.cells))
    out_ref[...] = res.reshape(sz.c, SLAB, sz.cells).astype(BF)


def skip_stage(sz, gs, weight):
    eye = jnp.eye(SLAB, dtype=BF)
    n = sz.c * SLAB
    row = lax.broadcasted_iota(jnp.int32, (n, n), 0)
    col = lax.broadcasted_iota(jnp.int32, (n, n), 1)
    spread = jnp.repeat(jnp.repeat(weight.T, SLAB, 0), SLAB, 1)
    mat = jnp.where(row % SLAB == col % SLAB, spread, jnp.zeros((), BF))
    return pl.pallas_call(
        functools.partial(skip_kernel, sz, len(gs)),
        grid=(sz.rows // SLAB,),
        in_specs=[
            pl.BlockSpec((g.shape[0], SLAB, sz.cells), lambda i: (0, i, 0)) for g in gs
        ]
        + [full((n, n))],
        out_specs=pl.BlockSpec((sz.c, SLAB, sz.cells), lambda i: (0, i, 0)),
        out_shape=jax.ShapeDtypeStruct((sz.c, sz.rows, sz.cells), BF),
        compiler_params=params(),
        cost_estimate=cost(2 * n * n * sz.cells * sz.rows // SLAB, 4 * sz.c * sz.rows * sz.cells),
        name="skip_map",
    )(*gs, mat)


def x_kernel(sz, cc, *refs):
    ins, table_ref = parts_of(refs)[: sz.na], refs[sz.ca]
    outs = parts_of(refs[sz.ca + 1 :])
    x = jnp.concatenate([r[p] for r in ins for p in range(2)], 1)
    res = nn_dot(x, table_ref[...])
    half = cc * sz.m // 2
    w = 2 * sz.kx * sz.yl
    for b in range(sz.nb):
        both = [res[:half, b * w : (b + 1) * w], res[half:, b * w : (b + 1) * w]]
        outs[b][...] = jnp.concatenate(both, 1).astype(BF)


def x_stage(sz, cc, pieces, table):
    w = 2 * sz.kx * sz.yl
    return list(
        pl.pallas_call(
            functools.partial(x_kernel, sz, cc),
            in_specs=[VM] * (sz.ca + 1),
            out_specs=[VM] * sz.cb,
            out_shape=shapes_of(sz.nb, (cc * sz.m // 2, 2 * w)),
            compiler_params=params(16),
            cost_estimate=cost(2 * cc * sz.m * table.shape[0] * table.shape[1], 8 << 20),
            name="x_forward",
        )(*pieces, table)
    )


def x_back_kernel(sz, cc, *refs):
    ins, table_ref = parts_of(refs)[: sz.nb], refs[sz.cb]
    outs = parts_of(refs[sz.cb + 1 :])
    w = 2 * sz.kx * sz.yl
    half = cc * sz.m // 2
    table = table_ref[...]
    for h in range(2):
        x = jnp.concatenate([r[:, h * w : (h + 1) * w] for r in ins], 1)
        res = nt_dot(x, table) * (1.0 / NX)
        for d in range(sz.na):
            for p in range(2):
                k = (d * 2 + p) * sz.rows
                outs[d][p, h * half : (h + 1) * half, :] = res[:, k : k + sz.rows].astype(BF)


def x_back_stage(sz, cc, pieces, table):
    return list(
        pl.pallas_call(
            functools.partial(x_back_kernel, sz, cc),
            in_specs=[VM] * (sz.cb + 1),
            out_specs=[VM] * sz.ca,
            out_shape=shapes_of(sz.na, (2, cc * sz.m, sz.rows)),
            compiler_params=params(16),
            cost_estimate=cost(2 * cc * sz.m * table.shape[0] * table.shape[1], 8 << 20),
            name="x_backward",
        )(*pieces, table)
    )


ROWS = 16
LANES = 128


def tiles(width):
    return -(-width // LANES)


def put_rows(ref, start, value):
    width = value.shape[1]
    pad = tiles(width) * LANES - width
    if pad:
        value = jnp.concatenate([value, jnp.zeros((value.shape[0], pad), value.dtype)], 1)
    for t in range(tiles(width)):
        ref[(t,) + start] = value[:, t * LANES : (t + 1) * LANES]


def get_rows(ref, start):
    return jnp.concatenate([ref[(t,) + start] for t in range(ref.shape[0])], 1)


def spans(lo, width):
    out = []
    while width:
        t, at = lo // LANES, lo % LANES
        n = min(width, LANES - at)
        out.append((t, at, n))
        lo, width = lo + n, width - n
    return out


PERIOD = LANES // math.gcd(KY, LANES)
PERIOD_TILES = PERIOD * KY // LANES


def over_modes(sz, body):
    def loop(j, _):
        for r in range(PERIOD):
            body(j * PERIOD + r, j * PERIOD_TILES, r)
        return 0

    whole_periods = sz.m // PERIOD
    if whole_periods:
        lax.fori_loop(0, whole_periods, loop, 0)
    for r in range(sz.m % PERIOD):
        body(whole_periods * PERIOD + r, whole_periods * PERIOD_TILES, r)


def to_lanes(sz, s_ref, z_ref, count):
    def body(m, tile, r):
        x = get_rows(s_ref, (pl.ds(m, count, sz.m), slice(None)))
        for k in range(4 * sz.kx):
            at = k * KY
            for t, lo, n in spans(r * KY, KY):
                rows = slice(k * ROWS, k * ROWS + count)
                z_ref[tile + t, rows, lo : lo + n] = x[:, at : at + n]
                at += n

    over_modes(sz, body)


def from_lanes(sz, z_ref, s_ref, count):
    def body(m, tile, r):
        parts = [
            z_ref[tile + t, k * ROWS : k * ROWS + count, lo : lo + n]
            for k in range(4 * sz.kx)
            for t, lo, n in spans(r * KY, KY)
        ]
        put_rows(s_ref, (pl.ds(m, count, sz.m), slice(None)), jnp.concatenate(parts, 1))

    over_modes(sz, body)


def places(sz):
    where, base = {}, 0
    for off, cc in sz.chunks:
        for j in range(cc):
            where[off + j] = (j // (cc // 2), base + j % (cc // 2))
        base += cc // 2
    return where


def load_spectrum(sz, ins, table_ref, s_ref, z_ref, d_ref):
    base = 0
    for k, (_, cc) in enumerate(sz.chunks):
        rows = cc * sz.m // 2
        pieces = parts_of(ins[k * sz.cb : (k + 1) * sz.cb])
        x = jnp.concatenate([r[...] for r in pieces], 1)
        put_rows(s_ref, (slice(base, base + rows), slice(None)), nn_dot(x, table_ref[...]))
        base += rows
    z_ref[...] = jnp.zeros(z_ref.shape, F32)
    to_lanes(sz, s_ref, z_ref, sz.c // 2)
    for o, (h, r) in places(sz).items():
        for q in range(2):
            for t in range(tiles(sz.m * KY)):
                rows = pl.ds(((2 * h + q) * sz.kx) * ROWS + r, SUB, ROWS)
                d_ref[q, t, o] = z_ref[t, rows, :]


def mixed(sz, d_ref, weight_of, t, fields):
    acc = [None] * fields
    for o in range(sz.c):
        sr, si = d_ref[0, t, o], d_ref[1, t, o]
        for f in range(fields):
            wr, wi = weight_of(0, o, f, t), weight_of(1, o, f, t)
            re = sr * wr + si * wi
            im = si * wr - sr * wi
            acc[f] = (re, im) if acc[f] is None else (acc[f][0] + re, acc[f][1] + im)
    return acc


FIELDS = 4


def mix_kernel(sz, *refs):
    n_in = len(sz.chunks) * sz.cb
    ins = refs[:n_in]
    table_ref, w_ref = refs[n_in : n_in + 2]
    outs = refs[n_in + 2 : n_in + 2 + n_in]
    s_ref, z_ref, d_ref, z2_ref = refs[n_in + 2 + n_in :]
    i = pl.program_id(0)
    where = places(sz)

    @pl.when(i == 0)
    def _():
        load_spectrum(sz, ins, table_ref, s_ref, z_ref, d_ref)

    def weight_of(p, o, f, t):
        return w_ref[p, o, f, :, t * LANES : (t + 1) * LANES].astype(F32)

    starts = []
    for f in range(FIELDS):
        at = jnp.int32(0)
        for step in range(sz.c // FIELDS):
            h, r = where[step * FIELDS + f]
            at = jnp.where(i == step, 2 * h * sz.kx * ROWS + r, at)
        starts.append(at)
    for t in range(tiles(sz.m * KY)):
        for f, (re, im) in enumerate(mixed(sz, d_ref, weight_of, t, FIELDS)):
            z2_ref[t, pl.ds(starts[f], sz.kx, ROWS), :] = re[: sz.kx]
            z2_ref[t, pl.ds(starts[f] + sz.kx * ROWS, sz.kx, ROWS), :] = im[: sz.kx]

    @pl.when(i == sz.c // FIELDS - 1)
    def _():
        from_lanes(sz, z2_ref, s_ref, sz.c // 2)
        w = 4 * sz.kx * sz.yl
        base = 0
        for k, (_, cc) in enumerate(sz.chunks):
            rows = cc * sz.m // 2
            x = get_rows(s_ref, (slice(base, base + rows), slice(None)))
            x = x[:, : table_ref.shape[1]].astype(BF)
            res = nt_dot(x, table_ref[...]) * (1.0 / NY)
            pieces = parts_of(outs[k * sz.cb : (k + 1) * sz.cb])
            for r in range(sz.nb):
                pieces[r][...] = res[:, r * w : (r + 1) * w].astype(BF)
            base += rows


SUB = 8


def y_scratch(sz):
    lanes = 4 * sz.kx * KY
    wide = tiles(sz.m * KY)
    z = pltpu.VMEM((wide, (4 * sz.kx + SUB) * ROWS, LANES), F32)
    return [
        pltpu.VMEM((tiles(lanes), sz.c // 2 * sz.m, LANES), F32),
        z,
        pltpu.VMEM((2, wide, sz.c, SUB, LANES), F32),
        z,
    ]


def pad_tiles(sz, weights):
    lead = [(0, 0)] * (weights.ndim - 2)
    over = tiles(sz.m * KY) * LANES - weights.shape[-1]
    return jnp.pad(weights, lead + [(0, SUB - sz.kx), (0, over)])


def mix_stage(sz, pieces, table, weights):
    modes = weights.shape[-1]
    outs = []
    for _, cc in sz.chunks:
        outs += shapes_of(sz.nb, (cc * sz.m // 2, 4 * sz.kx * sz.yl))
    res = pl.pallas_call(
        functools.partial(mix_kernel, sz),
        grid=(sz.c // FIELDS,),
        in_specs=[VM] * (len(pieces) + 1)
        + [pl.BlockSpec((2, sz.c, FIELDS, SUB, modes), lambda i: (0, 0, i, 0, 0))],
        out_specs=[VM] * len(outs),
        out_shape=outs,
        scratch_shapes=y_scratch(sz),
        compiler_params=params(24),
        cost_estimate=cost(20e9, 12 << 20),
        name="y_mix",
    )(*pieces, table, weights)
    n = sz.cb
    return [list(res[k * n : (k + 1) * n]) for k in range(len(sz.chunks))]


def mix_last_kernel(sz, *refs):
    n_in = len(sz.chunks) * sz.cb
    ins = refs[:n_in]
    table_ref, w_ref = refs[n_in : n_in + 2]
    outs = refs[n_in + 2 : n_in + 2 + sz.cb]
    s_ref, z_ref, d_ref, z2_ref = refs[n_in + 2 + sz.cb :]
    load_spectrum(sz, ins, table_ref, s_ref, z_ref, d_ref)

    def weight_of(p, o, f, t):
        return w_ref[p, o, :, t * LANES : (t + 1) * LANES]

    z2_ref[...] = jnp.zeros(z2_ref.shape, F32)
    for t in range(tiles(sz.m * KY)):
        re, im = mixed(sz, d_ref, weight_of, t, 1)[0]
        z2_ref[t, pl.ds(0, sz.kx, ROWS), :] = re[: sz.kx]
        z2_ref[t, pl.ds(sz.kx * ROWS, sz.kx, ROWS), :] = im[: sz.kx]
    from_lanes(sz, z2_ref, s_ref, 1)
    w = 4 * sz.kx * sz.yl
    x = get_rows(s_ref, (slice(0, sz.m), slice(None)))[:, : table_ref.shape[1]]
    res = nt_dot(x.astype(BF), table_ref[...]) * (1.0 / NY)
    pieces = parts_of(outs)
    for r in range(sz.nb):
        pieces[r][...] = res[:, r * w : (r + 1) * w].astype(BF)


def mix_last_stage(sz, pieces, table, folded):
    return list(
        pl.pallas_call(
            functools.partial(mix_last_kernel, sz),
            in_specs=[VM] * (len(pieces) + 2),
            out_specs=[VM] * sz.cb,
            out_shape=shapes_of(sz.nb, (sz.m, 4 * sz.kx * sz.yl)),
            scratch_shapes=y_scratch(sz),
            compiler_params=params(24),
            cost_estimate=cost(4e9, 4 << 20),
            name="y_mix_last",
        )(*pieces, table, folded)
    )


def gather_modes(sz, ins, k):
    parts = [
        r[p].astype(F32)[k * sz.m : (k + 1) * sz.m] for r in ins for p in range(2)
    ]
    return jnp.concatenate(parts, 0)


def next_kernel(sz, v_ref, *refs):
    n = sz.ca
    ins = parts_of(refs[:n])
    skip_ref, pre_ref, table_ref, part_ref = refs[n : n + 4]
    proj_ref = refs[n + 4]
    outs = parts_of(refs[n + 5 : n + 5 + n])
    f_ref, g_ref = refs[n + 5 + n :]
    step = pl.program_id(0)
    modes = jnp.concatenate([gather_modes(sz, ins, k) for k in range(sz.g)], 1)
    f_ref[...] = nn_dot(modes.T.astype(BF), table_ref[...]) * (1.0 / sz.cells)

    @pl.when(step == 0)
    def _():
        proj_ref[...] = part_ref[...]

    for k in range(sz.g):
        scale = v_ref[step * sz.g + k]

        def slab(j, _, k=k, scale=scale):
            s = pl.ds(pl.multiple_of(j * SLAB, SLAB), SLAB)
            fs = pl.ds(pl.multiple_of(k * sz.rows + j * SLAB, SLAB), SLAB)
            inc = f_ref[fs, :] + skip_ref[k, s, :].astype(F32)
            g = (inc * slope_of(pre_ref[0, k, s, :].astype(F32))).astype(BF)
            g_ref[fs, :] = g
            proj_ref[s, :] += scale * g.astype(F32)
            return 0

        lax.fori_loop(0, sz.rows // SLAB, slab, 0)
    emit_spectrum(sz, g_ref[...], table_ref, outs)


def next_stage(sz, chunk, pieces, skip, pre, layer, table, lift_skip, partial_proj):
    off, cc = chunk
    o = off // sz.g
    blk = (sz.g, sz.rows, sz.cells)
    pspecs = specs_of(sz.na, (2, sz.g * sz.m, sz.rows))
    plane = (sz.rows, sz.cells)
    res = pl.pallas_call(
        functools.partial(next_kernel, sz),
        grid=(cc // sz.g,),
        in_specs=[pl.BlockSpec(memory_space=pltpu.SMEM)]
        + pspecs
        + [
            pl.BlockSpec(blk, lambda i: (i + o, 0, 0)),
            pl.BlockSpec((1,) + blk, lambda i: (layer, i + o, 0, 0)),
            full(table.shape),
            full(plane),
        ],
        out_specs=[full(plane)] + pspecs,
        out_shape=[jax.ShapeDtypeStruct(plane, F32)]
        + shapes_of(sz.na, (2, cc * sz.m, sz.rows)),
        scratch_shapes=[
            pltpu.VMEM((sz.g * sz.rows, sz.cells), F32),
            pltpu.VMEM((sz.g * sz.rows, sz.cells), BF),
        ],
        compiler_params=params(),
        cost_estimate=cost(2 * cc * sz.rows * sz.cells * 1300, 6 * cc * sz.rows * sz.cells),
        name="next_zt",
    )(lift_skip[off : off + cc], *pieces, skip, pre, table, partial_proj)
    return res[0], list(res[1:])


def final_kernel(sz, *refs):
    ins = parts_of(refs[: sz.ca])
    table_ref, proj_ref, out_ref = refs[sz.ca :]
    modes = gather_modes(sz, ins, 0)
    spectral = nn_dot(modes.T.astype(BF), table_ref[...]) * (1.0 / sz.cells)
    out_ref[...] = spectral + proj_ref[...]


def final_stage(sz, pieces, table, proj):
    return pl.pallas_call(
        functools.partial(final_kernel, sz),
        in_specs=[VM] * (sz.ca + 2),
        out_specs=VM,
        out_shape=jax.ShapeDtypeStruct((sz.rows, sz.cells), F32),
        compiler_params=params(),
        cost_estimate=cost(1e9, 6 << 20),
        name="final_zt",
    )(*pieces, table, proj)


def exchange(pieces, axis):
    n = len(pieces)
    out = [pieces[0]]
    for d in range(1, n):
        out.append(lax.ppermute(pieces[d], axis, [(k, k ^ d) for k in range(n)]))
    return out


def partner(axis, d):
    return jnp.bitwise_xor(lax.axis_index(axis), jnp.asarray(d, jnp.int32))


def plane_kernel(sz, index_ref, small_ref, out_ref):
    place = lax.broadcasted_iota(jnp.int32, (2 * NZ, sz.cells), 0) % NZ
    cell = lax.broadcasted_iota(jnp.int32, (2 * NZ, sz.cells), 1)
    pick_z = jnp.where(place == cell // NT, 1.0, 0.0).astype(BF)
    pick_t = jnp.where(place == cell % NT, 1.0, 0.0).astype(BF)
    rows = jnp.concatenate([small_ref[jnp.bitwise_xor(index_ref[0], d)] for d in range(sz.na)], 0)
    w = 2 * NZ
    f = [
        nn_dot(rows[:, k * w : (k + 1) * w].astype(BF), pick)
        for k, pick in enumerate([pick_z, pick_t, pick_z, pick_t])
    ]
    out_ref[...] = (f[0] * f[1] + f[2] * f[3]).astype(BF)


def plane_blocks(sz):
    small = plane_factors()
    base = small.reshape(2, sz.na, sz.m, small.shape[-1]).transpose(1, 0, 2, 3)
    const = jnp.asarray(base.reshape(sz.na, 2 * sz.m, small.shape[-1]), BF)
    index = lax.axis_index("aa").astype(jnp.int32).reshape(1)
    return pl.pallas_call(
        functools.partial(plane_kernel, sz),
        in_specs=[pl.BlockSpec(memory_space=pltpu.SMEM), VM],
        out_specs=VM,
        out_shape=jax.ShapeDtypeStruct((sz.na * 2 * sz.m, sz.cells), BF),
        compiler_params=params(40),
        cost_estimate=cost(3e9, 4 << 20),
        name="plane_table",
    )(index, const)


def spread_dot(left, small, right, keep):
    wide = nn_dot(nn_dot(left, small).astype(BF), right)
    return jnp.where(keep, wide, 0.0).astype(BF)


def x_table(sz):
    small = jnp.asarray(line_table(KX, NX).reshape(2 * NX, 2 * KX), BF)
    n, w = sz.na * 2 * sz.rows, sz.nb * 2 * sz.kx * sz.yl
    row = np.arange(n)
    d, p, x = row // (2 * sz.rows), row // sz.rows % 2, row // sz.yl % sz.xl
    place = p * NX + partner("aa", d) * sz.xl + x
    left = (place[:, None] == jnp.arange(2 * NX)[None, :]).astype(BF)
    col = np.arange(w)
    b, q = col // (2 * sz.kx * sz.yl), col // (sz.kx * sz.yl) % 2
    k = col // sz.yl % sz.kx
    freq = q * KX + partner("ba", b) * sz.kx + k
    right = (jnp.arange(2 * KX)[:, None] == freq[None, :]).astype(BF)
    keep = (jnp.arange(n) % sz.yl)[:, None] == (jnp.arange(w) % sz.yl)[None, :]
    return spread_dot(left, small, right, keep)


def y_table(sz, zero):
    small = jnp.asarray(line_table(KY, NY).reshape(2 * NY, 2 * KY), BF) + zero
    part = sz.kx * sz.yl
    n, w = sz.nb * 4 * part, 4 * sz.kx * KY
    row = np.arange(n)
    r, h, q = row // (4 * part), row // (2 * part) % 2, row // part % 2
    kx, y = row // sz.yl % sz.kx, row % sz.yl
    place = q * NY + partner("ba", r) * sz.yl + y
    left = (place[:, None] == jnp.arange(2 * NY)[None, :]).astype(BF)
    col = np.arange(w)
    h2, q2 = col // (2 * sz.kx * KY), col // (sz.kx * KY) % 2
    kx2, ky = col // KY % sz.kx, col % KY
    freq = jnp.asarray(q2 * KY + ky, jnp.int32)
    right = (jnp.arange(2 * KY)[:, None] == freq[None, :]).astype(BF)
    group = jnp.asarray(h * sz.kx + kx, jnp.int32)
    group2 = jnp.asarray(h2 * sz.kx + kx2, jnp.int32)
    return spread_dot(left, small, right, group[:, None] == group2[None, :])


def whole(cotangent, pre_activations, spectral_weights, skip_weights, lift_weights):
    layers, _, channels, xl, yl, cells = pre_activations.shape
    sz = Sizes(channels, lax.axis_size("aa"), lax.axis_size("ba"))
    plane = plane_blocks(sz)
    tx = x_table(sz)
    pre = pre_activations.reshape(layers, channels, xl * yl, cells)
    cot = cotangent.reshape(channels, xl * yl, cells)
    lift_skip = jnp.sum(skip_weights[0].astype(F32) * lift_weights[None, :], axis=1)

    gs, spectra = [], []
    after = lift_skip
    for chunk in sz.chunks:
        g, pieces = first_stage(sz, chunk, cot, pre, 1, plane, after)
        after = g
        gs.append(g)
        spectra.append(exchange(pieces, "aa"))
    skip = skip_stage(sz, gs, skip_weights[1])

    moved = []
    for (_, cc), pieces in zip(sz.chunks, spectra):
        out = x_stage(sz, cc, pieces, tx)
        moved.append(exchange(out, "ba"))
        last_out = out[0]
    raw, zero, _ = lax.optimization_barrier(
        (spectral_weights[1].transpose(1, 2, 3, 0, 4), jnp.zeros((), BF), last_out)
    )
    weights = pad_tiles(sz, raw.transpose(3, 0, 1, 2, 4))
    ty = y_table(sz, zero)
    modes = mix_stage(sz, sum(moved, []), ty, weights)

    back = [exchange(pieces, "ba") for pieces in modes]
    for j, ((_, cc), pieces) in enumerate(zip(sz.chunks, back)):
        out = x_back_stage(sz, cc, pieces, tx)
        back[j] = exchange(out, "aa")

    lift = lift_weights[None, None, :, None, None]
    folded = pad_tiles(sz, jnp.sum(spectral_weights[0].astype(F32) * lift, axis=2))
    proj = jnp.zeros((sz.rows, cells), F32)
    spectra = []
    for chunk, pieces in zip(sz.chunks, back):
        proj, out = next_stage(sz, chunk, pieces, skip, pre, 0, plane, lift_skip, proj)
        spectra.append(exchange(out, "aa"))

    moved = []
    for (_, cc), pieces in zip(sz.chunks, spectra):
        out = x_stage(sz, cc, pieces, tx)
        moved += exchange(out, "ba")
    last = exchange(mix_last_stage(sz, moved, ty, folded), "ba")
    last = exchange(x_back_stage(sz, 2, last, tx), "aa")
    out = final_stage(sz, last, plane, proj)
    return out.reshape(1, xl, yl, cells)


def solution(mesh):
    return jax.shard_map(
        whole,
        mesh=mesh,
        in_specs=(
            P(None, None, "aa", "ba", None),
            P(None, None, None, "aa", "ba", None),
            P(None, None, None, None, "ba", "aa"),
            P(),
            P(),
        ),
        out_specs=P(None, "aa", "ba", None),
        check_vma=False,
    )
```
